256 devices in a mesh: ctx: 64 (over y, z, core), head: 4 (over x).
Axes of the slice: x: 4, y: 4, z: 8, core: 2. Of those that a mesh axis runs over, the one named last changes fastest.
Arguments:
- block_order: int32 [128], replicated, may hold values from 0 to 127, as said below
- main_query: bfloat16 [8192, 36864], P('ctx', 'head'), may hold values from -256 to 256
- latent_key: bfloat16 [576, 8192], P(None, 'ctx'), may hold values from -24 to 24
- index_query: bfloat16 [8192, 32, 128], P('ctx', 'head'), may hold values from -64 to 64
- index_weight: bfloat16 [8192, 32], P('ctx', 'head'), may hold values from -0.6 to 0.6
- index_key: bfloat16 [128, 8192], P(None, 'ctx'), may hold values from -24 to 24
Outputs:
- row_loss: float32 [8192], P('ctx')
- grad_query: bfloat16 [8192, 32, 128], P('ctx', 'head')
- grad_weight: bfloat16 [8192, 32], P('ctx', 'head')
- grad_key: float32 [8192, 128], P(('ctx', 'head'))
The draws below stay inside these ranges and needn't reach their ends.
Inputs may be any that keep to these rules, and one draw needn't show every extreme that they name: `block_order`: slots 2d and 2d+1 hold blocks s * 64 + c and s * 64 + 128 // 2 - 1 - c of one sequence s, for some c below 32, and every block appears once.
All inputs are finite; a program needn't handle non-finite values.
Results may differ from the reference program's by a relative error of at most 0.01.
Values may be sent and summed in bfloat16 or wider, within the bound.
No kernel may reach another device: no remote copies, remote signals or barrier semaphores. Data moves between devices by JAX's collectives and lax.ppermute only.
A program may use at most 128 MiB of HBM per device.

```python
import math
import jax
import jax.numpy as jnp
from jax import lax

BLOCK = 64
HM = 64
KW = 576
HEAD_QK = 192
HI = 32
DI = 128
BLOCKS = 128
LENGTH = 4096
SEQ = 8192


def drawn_rows(key):
    offsets = jax.random.randint(jax.random.fold_in(key, 11), (BLOCKS,), 1, BLOCK)
    chosen_rows = jnp.arange(BLOCKS, dtype=jnp.int32) * BLOCK + offsets.astype(jnp.int32)
    level = (jnp.arange(BLOCKS, dtype=jnp.int32) % 3).astype(jnp.float32)
    target_score = 120.0 + 105.0 * level
    gap_size = 1.0 + level
    return (chosen_rows, target_score, gap_size)


def draw_block_order(key, part):
    pair_count = BLOCKS // 2
    half_pairs = pair_count // 2
    chosen = jax.random.permutation(jax.random.fold_in(key, 1), pair_count).astype(jnp.int32)
    sequence_id = chosen // half_pairs
    inner = chosen % half_pairs
    early_blocks = sequence_id * pair_count + inner
    late_blocks = sequence_id * pair_count + pair_count - 1 - inner
    return jnp.stack([early_blocks, late_blocks], axis=1).reshape(BLOCKS).astype(jnp.int32)


def draw_latent_key(key, part):
    values_drawn = jax.random.normal(jax.random.fold_in(key, 2), (KW, SEQ), jnp.float32)
    chosen_rows, target_score, gap_size = drawn_rows(key)
    anchor = 4.0 * jax.random.normal(jax.random.fold_in(key, 14), (KW, BLOCKS), jnp.float32)
    anchor = jnp.clip(anchor, -24.0, 24.0)
    spread_size = jnp.sqrt(jnp.mean(anchor * anchor, axis=0, keepdims=True))
    noise = jax.random.normal(jax.random.fold_in(key, 4), (KW, BLOCKS), jnp.float32)
    near_copy = anchor * (1.0 - gap_size / target_score)[None, :] + 0.005 * spread_size * noise
    values_drawn = values_drawn.at[:, chosen_rows].set(anchor)
    values_drawn = values_drawn.at[:, chosen_rows - 1].set(near_copy)
    return jnp.clip(values_drawn, -24.0, 24.0).astype(jnp.bfloat16)


def draw_main_query(key, part):
    values_drawn = jax.random.normal(jax.random.fold_in(key, 5), (SEQ, HM, KW), jnp.float32)
    keys_float = draw_latent_key(key, part).astype(jnp.float32)
    chosen_rows, target_score, gap_size = drawn_rows(key)
    anchor = keys_float[:, chosen_rows].T
    factor = target_score * math.sqrt(HEAD_QK)
    aligned = factor[:, None] * anchor / jnp.sum(anchor * anchor, axis=1, keepdims=True)
    values_drawn = values_drawn.at[chosen_rows].set(jnp.broadcast_to(aligned[:, None, :], (BLOCKS, HM, KW)))
    return jnp.clip(values_drawn, -256.0, 256.0).reshape(SEQ, HM * KW).astype(jnp.bfloat16)


def draw_index_key(key, part):
    values_drawn = jax.random.normal(jax.random.fold_in(key, 7), (DI, SEQ), jnp.float32)
    chosen_rows, target_score, gap_size = drawn_rows(key)
    anchor = 4.0 * jax.random.normal(jax.random.fold_in(key, 15), (DI, BLOCKS), jnp.float32)
    anchor = jnp.clip(anchor, -24.0, 24.0)
    spread_size = jnp.sqrt(jnp.mean(anchor * anchor, axis=0, keepdims=True))
    noise = jax.random.normal(jax.random.fold_in(key, 12), (DI, BLOCKS), jnp.float32)
    near_copy = anchor * (1.0 - gap_size / target_score)[None, :] + 0.005 * spread_size * noise
    values_drawn = values_drawn.at[:, chosen_rows].set(anchor)
    values_drawn = values_drawn.at[:, chosen_rows - 1].set(near_copy)
    return jnp.clip(values_drawn, -24.0, 24.0).astype(jnp.bfloat16)


def draw_index_weight(key, part):
    values_drawn = 0.1 * jax.random.normal(jax.random.fold_in(key, 9), (SEQ, HI), jnp.float32)
    return jnp.clip(values_drawn, -0.6, 0.6).astype(jnp.bfloat16)


def draw_index_query(key, part):
    values_drawn = jax.random.normal(jax.random.fold_in(key, 10), (SEQ, HI, DI), jnp.float32)
    keys_float = draw_index_key(key, part).astype(jnp.float32)
    weights = draw_index_weight(key, part).astype(jnp.float32)
    chosen_rows, target_score, gap_size = drawn_rows(key)
    anchor = keys_float[:, chosen_rows].T
    unit_part = anchor / jnp.sum(anchor * anchor, axis=1, keepdims=True)
    chosen_weights = weights[chosen_rows]
    signs = jnp.sign(chosen_weights)
    weight_total = jnp.sum(jnp.abs(chosen_weights), axis=1) + 0.001
    factor = target_score / weight_total
    aligned = factor[:, None, None] * signs[:, :, None] * unit_part[:, None, :]
    values_drawn = values_drawn.at[chosen_rows].set(aligned)
    return jnp.clip(values_drawn, -64.0, 64.0).astype(jnp.bfloat16)


def setup_inputs(seed: int = 0) -> dict:
    key_of = jax.random.split(jax.random.key(seed), 7)
    block_order = draw_block_order(jax.random.fold_in(key_of[6], 71), 0)
    main_query = draw_main_query(jax.random.fold_in(key_of[6], 71), 0)
    latent_key = draw_latent_key(jax.random.fold_in(key_of[6], 71), 0)
    index_query = draw_index_query(jax.random.fold_in(key_of[6], 71), 0)
    index_weight = draw_index_weight(jax.random.fold_in(key_of[6], 71), 0)
    index_key = draw_index_key(jax.random.fold_in(key_of[6], 71), 0)
    return dict(block_order=block_order, main_query=main_query, latent_key=latent_key, index_query=index_query, index_weight=index_weight, index_key=index_key)


masked_value = -1e+30

def reference(block_order, main_query, latent_key, index_query, index_weight, index_key):
    slot_of = jnp.argsort(block_order).astype(jnp.int32)
    offsets = jnp.arange(BLOCK, dtype=jnp.int32)
    row_sorted = (slot_of[:, None] * BLOCK + offsets[None, :]).reshape(SEQ)
    row_stored = (block_order.astype(jnp.int32)[:, None] * BLOCK + offsets[None, :]).reshape(SEQ)
    queries = main_query[row_sorted].reshape(SEQ, HM, KW)
    latent = latent_key[:, row_sorted]
    index_rows = index_query[row_sorted]
    index_weights = index_weight[row_sorted].astype(jnp.float32)
    index_keys = index_key[:, row_sorted]
    score_scale = 1.0 / math.sqrt(HEAD_QK)
    row_block = math.gcd(LENGTH, 512)
    key_grad = jnp.zeros((SEQ, DI), jnp.float32)
    loss_parts = []
    query_parts = []
    weight_parts = []
    for block_index in range(SEQ // row_block):
        first_row = block_index * row_block
        last_row = first_row + row_block
        key_first = first_row // LENGTH * LENGTH
        key_lat = latent[:, key_first:last_row]
        key_idx = index_keys[:, key_first:last_row]
        row_pos = first_row + jnp.arange(row_block, dtype=jnp.int32)
        visible = (key_first + jnp.arange(last_row - key_first, dtype=jnp.int32))[None, :] <= row_pos[:, None]

        def add_head(target_sum, query_rows):
            scores = jnp.dot(query_rows, key_lat, preferred_element_type=jnp.float32) * score_scale
            scores = jnp.where(visible, scores, masked_value)
            top_score = lax.optimization_barrier(jnp.max(scores, axis=1, keepdims=True))
            raised = jnp.exp(scores - top_score)
            return (target_sum + raised / lax.optimization_barrier(jnp.sum(raised, axis=1, keepdims=True)), None)
        target, unused = lax.scan(add_head, jnp.zeros((row_block, last_row - key_first), jnp.float32), jnp.moveaxis(queries[first_row:last_row], 1, 0))
        target = target * (1.0 / HM)
        head_rows = jnp.moveaxis(index_rows[first_row:last_row], 1, 0)
        head_weights = jnp.moveaxis(index_weights[first_row:last_row], 1, 0)

        def add_index(logit_sum, paired):
            query_rows, weight_col = paired
            activation = jnp.dot(query_rows, key_idx, preferred_element_type=jnp.float32)
            return (logit_sum + weight_col[:, None] * jnp.maximum(activation, 0.0), None)
        logits, unused = lax.scan(add_index, jnp.zeros((row_block, last_row - key_first), jnp.float32), (head_rows, head_weights))
        masked = jnp.where(visible, logits, masked_value)
        top_logit = lax.optimization_barrier(jnp.max(masked, axis=1, keepdims=True))
        log_total = top_logit + jnp.log(lax.optimization_barrier(jnp.sum(jnp.exp(masked - top_logit), axis=1, keepdims=True)))
        loss_parts.append(lax.optimization_barrier(jnp.sum(jnp.where(visible, target * (log_total - logits), 0.0), axis=1)))
        slopes = jnp.where(visible, jnp.exp(masked - log_total) - target, 0.0).astype(jnp.bfloat16)
        slope_float = lax.optimization_barrier(slopes).astype(jnp.float32)

        def back_head(key_sum, triple):
            query_rows, weight_col = triple
            activation = jnp.dot(query_rows, key_idx, preferred_element_type=jnp.float32)
            grad_weight_col = lax.optimization_barrier(jnp.sum(slope_float * jnp.maximum(activation, 0.0), axis=1))
            through = jnp.where(activation > 0.0, slope_float * weight_col[:, None], 0.0).astype(jnp.bfloat16)
            grad_rows = jnp.dot(through, key_idx.T, preferred_element_type=jnp.float32)
            key_sum = key_sum + jnp.dot(through.T, query_rows, preferred_element_type=jnp.float32)
            return (key_sum, (grad_rows, grad_weight_col))
        key_sum, outputs = lax.scan(back_head, jnp.zeros((last_row - key_first, DI), jnp.float32), (head_rows, head_weights))
        key_grad = key_grad.at[key_first:last_row].add(key_sum)
        query_parts.append(jnp.moveaxis(outputs[0], 0, 1))
        weight_parts.append(jnp.moveaxis(outputs[1], 0, 1))
    row_loss = jnp.concatenate(loss_parts)[row_stored]
    grad_query = jnp.concatenate(query_parts)[row_stored].astype(jnp.bfloat16)
    grad_weight = jnp.concatenate(weight_parts)[row_stored].astype(jnp.bfloat16)
    grad_key = key_grad[row_stored]
    return (row_loss, grad_query, grad_weight, grad_key)
```

```python
import math

import jax
import jax.numpy as jnp
from jax import lax
from jax.experimental import pallas as pl
from jax.experimental.pallas import tpu as pltpu
from jax.sharding import Mesh
from jax.sharding import PartitionSpec as P

HM = 64
HI = 32
DI = 128
KW = 576
HEAD_QK = 192
BLOCK = 64
LENGTH = 4096
HALF = LENGTH // 2
CTX = ("ctx_0", "ctx_1", "ctx_2")
CTX_HEAD = ("ctx_0", "ctx_1", "ctx_2", "head")
HEADS = 4
GROUP = 16
MAIN_LANES = HM // HEADS * KW
INDEX_LANES = HI // HEADS * DI
ALL_LANES = MAIN_LANES + INDEX_LANES + 128
TILE = 256
TILES = LENGTH // TILE
PAIRS = LENGTH // TILE
ROWS = HM * GROUP
IROWS = HI * GROUP
KEY_ROWS = 1024
GRAD_ROWS = 9 * 2 * GROUP
masked_value = -1e30
SCORE_EXP2 = math.log2(math.e) / math.sqrt(HEAD_QK)
f32 = jnp.float32
bf16 = jnp.bfloat16


def nt_dot(a, b):
    return lax.dot_general(a, b, (((1,), (1,)), ((), ())), preferred_element_type=f32)


def rows_kernel(
    where_ref, meta_ref, gathered, q_ref, out_ref,
    raw, keys, q_all, qi_all, scores, best, total, w_all, target, logits, slope, gsum, key_grad, sems,
):
    c_own = meta_ref[0]
    h_own = meta_ref[1]

    def fetch(n):
        return pltpu.make_async_copy(gathered.at[where_ref[n]], raw.at[n], sems.at[n])

    for n in range(32):
        fetch(n).start()

    keys[0:64, :] = jnp.zeros((64, LENGTH), bf16)
    keys[640:704, :] = jnp.zeros((64, LENGTH), bf16)

    for e in range(2):
        for src in range(HEADS):
            for i in range(8):
                at = (src * 8 + i) * GROUP
                for parity in range(2):
                    lane = i * 2 * KW + parity * (KW - 64)
                    q_all[e, parity, at : at + GROUP, :] = q_ref[src, e, :, lane : lane + 640]
                lane = MAIN_LANES + i * DI
                qi_all[e, at : at + GROUP, :] = q_ref[src, e, :, lane : lane + DI]
                lane = MAIN_LANES + INDEX_LANES
                column = q_ref[src, e, :, lane : lane + 128].astype(f32)[:, i : i + 1]
                w_all[e, at : at + GROUP, :] = jnp.broadcast_to(column, (GROUP, DI))

    take = lax.broadcasted_iota(jnp.int32, (256, 256), 0)
    give = lax.broadcasted_iota(jnp.int32, (256, 256), 1)
    source = jnp.where(give // 64 == 1, give + 64, jnp.where(give // 64 == 2, give - 64, give))
    shuffle = jnp.where(take == source, 1.0, 0.0).astype(bf16)

    def sort_pair(i, carry):
        fetch(2 * i).wait()
        fetch(2 * i + 1).wait()
        both = jnp.concatenate([raw[2 * i], raw[2 * i + 1]], axis=1)
        mixed = jnp.dot(both, shuffle, preferred_element_type=f32).astype(bf16)
        early = pl.multiple_of(i * 128, 128)
        late = pl.multiple_of(HALF + i * 128, 128)
        keys[64:640, pl.ds(early, 128)] = mixed[0:KW, 0:128]
        keys[704:832, pl.ds(early, 128)] = mixed[KW:, 0:128]
        keys[64:640, pl.ds(late, 128)] = mixed[0:KW, 128:256]
        keys[704:832, pl.ds(late, 128)] = mixed[KW:, 128:256]
        return carry

    lax.fori_loop(0, 16, sort_pair, 0)

    key_grad[...] = jnp.zeros((DI, LENGTH), f32)

    for e in range(2):
        row_pos = lax.broadcasted_iota(jnp.int32, (GROUP, 1), 0) + h_own * GROUP
        row_pos = row_pos + (c_own if e == 0 else 63 - c_own) * BLOCK

        def key_pos(at, width):
            lane = lax.broadcasted_iota(jnp.int32, (1, width), 1) + at
            late_lane = lane - HALF
            late_pos = (63 - late_lane // BLOCK) * BLOCK + late_lane % BLOCK
            return jnp.where(lane < HALF, lane, late_pos)

        early_tiles = c_own // 4 + 1 if e == 0 else TILES // 2
        late_tiles = 0 if e == 0 else TILES // 2 - c_own // 4

        def tile_at(j):
            if e == 0:
                return pl.multiple_of(j * TILE, TILE)
            return pl.multiple_of(jnp.where(j < TILES // 2, j, j + c_own // 4) * TILE, TILE)

        steps = early_tiles + late_tiles

        best[...] = jnp.full((ROWS, 128), masked_value, f32)
        total[...] = jnp.zeros((ROWS, 128), f32)
        target[...] = jnp.zeros((GROUP, LENGTH), f32)
        logits[...] = jnp.full((GROUP, LENGTH), masked_value, f32)

        def score_step(j, carry):
            at = tile_at(j)
            visible = key_pos(at, TILE) <= row_pos
            for parity in range(2):
                k = keys[64 * (1 - parity) : 64 * (1 - parity) + 640, pl.ds(at, TILE)]
                s = jnp.dot(q_all[e, parity], k, preferred_element_type=f32)
                s = jnp.where(visible[None], s.reshape(HM // 2, GROUP, TILE), masked_value)
                s = s.reshape(ROWS // 2, TILE)
                r = slice(parity * (ROWS // 2), (parity + 1) * (ROWS // 2))
                scores[r, pl.ds(at, TILE)] = s
                best[r] = jnp.maximum(best[r], jnp.maximum(s[:, 0:128], s[:, 128:256]))
            return carry

        lax.fori_loop(0, steps, score_step, 0)

        def top_step(g, carry):
            r = pl.ds(pl.multiple_of(g * 128, 128), 128)
            best[r] = jnp.broadcast_to(jnp.max(best[r], axis=1, keepdims=True), (128, 128))
            return carry

        lax.fori_loop(0, ROWS // 128, top_step, 0)

        def exp_step(j, carry):
            at = tile_at(j)
            for g in range(ROWS // 128):
                r = slice(g * 128, (g + 1) * 128)
                top = best[r]
                part = total[r]
                for half in range(TILE // 128):
                    lanes = pl.ds(pl.multiple_of(at + half * 128, 128), 128)
                    raised = jnp.exp2((scores[r, lanes] - top) * SCORE_EXP2)
                    scores[r, lanes] = raised
                    part = part + raised
                total[r] = part
            return carry

        lax.fori_loop(0, steps, exp_step, 0)

        def total_step(g, carry):
            r = pl.ds(pl.multiple_of(g * 128, 128), 128)
            whole = jnp.sum(total[r], axis=1, keepdims=True)
            total[r] = jnp.broadcast_to((1.0 / HM) / whole, (128, 128))
            return carry

        lax.fori_loop(0, ROWS // 128, total_step, 0)

        def index_logits(at):
            act = jnp.dot(
                qi_all[e], keys[704:832, pl.ds(at, TILE)], preferred_element_type=f32
            )
            out = jnp.zeros((GROUP, TILE), f32)
            for h in range(HI):
                r = slice(h * GROUP, (h + 1) * GROUP)
                w = w_all[e, r]
                out = out + jnp.maximum(act[r], 0.0) * jnp.concatenate([w, w], axis=1)
            return out

        def target_step(j, carry):
            at = tile_at(j)
            lanes = pl.ds(at, TILE)
            acc = jnp.zeros((GROUP, TILE), f32)
            for h in range(HM):
                r = slice(h * GROUP, (h + 1) * GROUP)
                share = total[r]
                acc = acc + scores[r, lanes] * jnp.concatenate([share, share], axis=1)
            target[:, lanes] = acc
            visible = key_pos(at, TILE) <= row_pos
            logits[:, lanes] = jnp.where(visible, index_logits(at), masked_value)
            return carry

        lax.fori_loop(0, steps, target_step, 0)

        masked = logits[...]
        visible = masked > 0.5 * masked_value
        top_logit = jnp.max(masked, axis=1, keepdims=True)
        lse = top_logit + jnp.log(jnp.sum(jnp.exp(masked - top_logit), axis=1, keepdims=True))
        loss = jnp.sum(jnp.where(visible, target[...] * (lse - masked), 0.0), axis=1, keepdims=True)
        rounded = jnp.where(visible, jnp.exp(masked - lse) - target[...], 0.0).astype(bf16)
        slope[...] = rounded.astype(f32)

        gsum[...] = jnp.zeros((IROWS, DI), f32)
        q_float = qi_all[e].astype(f32)
        weighted = jnp.transpose(q_float * w_all[e]).astype(bf16)

        def back_step(j, carry):
            at = tile_at(j)
            lanes = pl.ds(at, TILE)
            k = keys[704:832, lanes]
            act = jnp.dot(qi_all[e], k, preferred_element_type=f32)
            through = jnp.where(
                act.reshape(HI, GROUP, TILE) > 0.0, slope[:, lanes][None], 0.0
            ).reshape(IROWS, TILE).astype(bf16)
            gsum[...] += nt_dot(through, k)
            key_grad[:, lanes] += jnp.dot(weighted, through, preferred_element_type=f32)
            return carry

        lax.fori_loop(0, steps, back_step, 0)

        grads = (gsum[...] * w_all[e]).astype(bf16)
        column = jnp.sum(gsum[...] * q_float, axis=1, keepdims=True)
        lane = lax.broadcasted_iota(jnp.int32, (GROUP, 128), 1)
        high = loss.astype(bf16).astype(f32)
        middle = (loss - high).astype(bf16).astype(f32)
        low = loss - high - middle
        extra = jnp.where(lane == 8, high, jnp.where(lane == 9, middle, jnp.where(lane == 10, low, 0.0)))
        for dst in range(HEADS):
            small = extra
            for i in range(8):
                at = (dst * 8 + i) * GROUP
                to = KEY_ROWS + (e * 9 + i) * GROUP
                out_ref[dst, to : to + GROUP, :] = grads[at : at + GROUP]
                small = jnp.where(lane == i, column[at : at + GROUP], small)
            to = KEY_ROWS + (e * 9 + 8) * GROUP
            out_ref[dst, to : to + GROUP, :] = small.astype(bf16)

    def emit(i, carry):
        for late in range(2):
            lanes = pl.ds(pl.multiple_of(late * HALF + i * 128, 128), 128)
            turned = jnp.transpose(key_grad[:, lanes]).astype(bf16)
            for k in range(4):
                to = pl.multiple_of(i * 64 + (k // 2) * 32, 32)
                out_ref[2 * late + k % 2, pl.ds(to, 32), :] = turned[k * 32 : (k + 1) * 32]
        return carry

    lax.fori_loop(0, 16, emit, 0)


def rows_call(where, meta, gathered, queries):
    return pl.pallas_call(
        rows_kernel,
        out_shape=jax.ShapeDtypeStruct((HEADS, KEY_ROWS + GRAD_ROWS, DI), bf16),
        in_specs=[
            pl.BlockSpec(memory_space=pltpu.SMEM),
            pl.BlockSpec(memory_space=pltpu.SMEM),
            pl.BlockSpec(memory_space=pl.ANY),
            pl.BlockSpec(memory_space=pltpu.VMEM),
        ],
        out_specs=pl.BlockSpec(memory_space=pltpu.VMEM),
        scratch_shapes=[
            pltpu.VMEM((32, KW + DI, 128), bf16),
            pltpu.VMEM((832, LENGTH), bf16),
            pltpu.VMEM((2, 2, ROWS // 2, 640), bf16),
            pltpu.VMEM((2, IROWS, DI), bf16),
            pltpu.VMEM((ROWS, LENGTH), f32),
            pltpu.VMEM((ROWS, 128), f32),
            pltpu.VMEM((ROWS, 128), f32),
            pltpu.VMEM((2, IROWS, DI), f32),
            pltpu.VMEM((GROUP, LENGTH), f32),
            pltpu.VMEM((GROUP, LENGTH), f32),
            pltpu.VMEM((GROUP, LENGTH), f32),
            pltpu.VMEM((IROWS, DI), f32),
            pltpu.VMEM((DI, LENGTH), f32),
            pltpu.SemaphoreType.DMA((32,)),
        ],
        compiler_params=pltpu.CompilerParams(vmem_limit_bytes=58 * 1024 * 1024),
        name="rows_work",
    )(where, meta, gathered, queries)


def spread_kernel(to_ref, got_ref, out_ref, sums):
    total = got_ref[0, 0:KEY_ROWS].astype(f32)
    for src in range(1, HEADS):
        total = total + got_ref[src, 0:KEY_ROWS].astype(f32)
    sums[0:KEY_ROWS] = total.astype(bf16)
    sums[KEY_ROWS:] = jnp.zeros((32, DI), bf16)

    def put(d, carry):
        out_ref[d] = sums[pl.ds(pl.multiple_of(to_ref[d] * 32, 32), 32)]
        return carry

    lax.fori_loop(0, 64, put, 0, unroll=8)


def spread_call(to, got):
    return pl.pallas_call(
        spread_kernel,
        out_shape=jax.ShapeDtypeStruct((64, 32, DI), bf16),
        in_specs=[
            pl.BlockSpec(memory_space=pltpu.SMEM),
            pl.BlockSpec(memory_space=pltpu.VMEM),
        ],
        out_specs=pl.BlockSpec(memory_space=pltpu.VMEM),
        scratch_shapes=[pltpu.VMEM((KEY_ROWS + 32, DI), bf16)],
        name="spread_keys",
    )(to, got)


def body(block_order, main_query, latent_key, index_query, index_weight, index_key):
    d_own = lax.axis_index(CTX)
    early = block_order.reshape(64, 2)[:, 0]
    own = lax.dynamic_index_in_dim(early, d_own, 0, keepdims=False)
    first = own // 64 * 64
    c_own = own - first
    slots = lax.iota(jnp.int32, 64)
    wanted = first + lax.iota(jnp.int32, 32)
    where = jnp.sum(jnp.where(early[None, :] == wanted[:, None], slots[None, :], 0), axis=1)
    to = jnp.where(early // 64 * 64 == first, early - first, 32)
    meta = jnp.stack([c_own, lax.axis_index("head")]).astype(jnp.int32)

    shard = jnp.concatenate([latent_key, index_key], axis=0)
    gathered = gather_keys(shard)

    weights = jnp.pad(index_weight, ((0, 0), (0, 128 - index_weight.shape[1])))
    rows = jnp.concatenate([main_query, index_query.reshape(128, INDEX_LANES), weights], axis=1)
    rows = rows.reshape(2, HEADS, GROUP, ALL_LANES).swapaxes(0, 1)
    queries = lax.all_to_all(rows, "head", split_axis=0, concat_axis=0, tiled=True)

    sent = rows_call(where, meta, gathered, queries)
    got = lax.all_to_all(sent, "head", split_axis=0, concat_axis=0, tiled=True)
    parts = lax.all_to_all(spread_call(to, got), CTX, split_axis=0, concat_axis=0, tiled=True)
    grad_key = jnp.sum(parts.astype(f32), axis=0)

    grads = got[:, KEY_ROWS:].reshape(HEADS, 2, 9, GROUP, DI).transpose(1, 0, 3, 2, 4)
    grads = grads.reshape(128, 9, DI)
    small = grads[:, 8]
    row_loss = jnp.sum(small[:, 8:11].astype(f32), axis=1)
    return (row_loss, grads[:, 0:8], small[:, 0:8], grad_key)


def gather_keys(shard):
    return lax.all_gather(shard, CTX)


def solution(mesh):
    split = Mesh(
        mesh.devices.reshape(4, 8, 2, mesh.shape["head"]), ("ctx_0", "ctx_1", "ctx_2", "head")
    )
    in_specs = (
        P(),
        P(CTX, "head"),
        P(None, CTX),
        P(CTX, "head", None),
        P(CTX, "head"),
        P(None, CTX),
    )
    out_specs = (P(CTX), P(CTX, "head", None), P(CTX, "head"), P(CTX_HEAD, None))
    return jax.shard_map(body, mesh=split, in_specs=in_specs, out_specs=out_specs, check_vma=False)
```

```python
import math

import jax
import jax.numpy as jnp
from jax import lax
from jax.experimental import pallas as pl
from jax.experimental.pallas import tpu as pltpu
from jax.sharding import Mesh
from jax.sharding import PartitionSpec as P

HM = 64
HI = 32
DI = 128
KW = 576
HEAD_QK = 192
BLOCK = 64
LENGTH = 4096
HALF = LENGTH // 2
CTX = ("ctx_0", "ctx_1", "ctx_2")
CTX_HEAD = ("ctx_0", "ctx_1", "ctx_2", "head")
HEADS = 4
GROUP = 16
MAIN_LANES = HM // HEADS * KW
INDEX_LANES = HI // HEADS * DI
ALL_LANES = MAIN_LANES + INDEX_LANES + 128
TILE = 256
TILES = LENGTH // TILE
PAIRS = LENGTH // TILE
ROWS = HM * GROUP
IROWS = HI * GROUP
KEY_ROWS = 1024
GRAD_ROWS = 9 * 2 * GROUP
HALF_ROWS = (KW + DI) // 2
STRIP = HALF_ROWS // 2
PIECES = 14
masked_value = -1e30
SCORE_EXP2 = math.log2(math.e) / math.sqrt(HEAD_QK)
f32 = jnp.float32
bf16 = jnp.bfloat16


def sources(y, z):
    if y == 2:
        a = (3, z) if z < 4 else (4, z - 4)
    else:
        a = ({0: 0, 1: 1, 3: 2}[y], z)
    if z == 4:
        b = (12, y) if y < 2 else (13, y - 2)
    else:
        b = ({0: 5, 1: 6, 2: 7, 3: 8, 5: 9, 6: 10, 7: 11}[z], y)
    return a, b


def nt_dot(a, b):
    return lax.dot_general(a, b, (((1,), (1,)), ((), ())), preferred_element_type=f32)


def rows_kernel(slot_ref, meta_ref, *refs):
    pieces = refs[: 2 * PIECES]
    q_ref, out_ref = refs[2 * PIECES : 2 * PIECES + 2]
    (
        raw, keys, q_all, qi_all, scores, best, total, w_all, target, logits, slope, gsum,
        key_grad, sems,
    ) = refs[2 * PIECES + 2 :]
    c_own = meta_ref[0]
    h_own = meta_ref[1]
    own_half = pl.multiple_of(meta_ref[2] * HALF_ROWS, 16)
    other_half = pl.multiple_of((1 - meta_ref[2]) * HALF_ROWS, 16)

    for y in range(4):
        for z in range(8):
            for core in range(2):
                slot = slot_ref[(y * 8 + z) * 2 + core]

                @pl.when(slot >= 0)
                def _():
                    for (piece, block), at in zip(sources(y, z), (0, STRIP)):
                        for kind, half in ((0, own_half), (1, other_half)):
                            pltpu.make_async_copy(
                                pieces[kind * PIECES + piece].at[block, core ^ kind],
                                raw.at[slot, pl.ds(half + at, STRIP), :],
                                sems.at[slot],
                            ).start()

    def arrived(n):
        pltpu.make_async_copy(raw.at[n], raw.at[n], sems.at[n]).wait()

    keys[0:64, :] = jnp.zeros((64, LENGTH), bf16)
    keys[640:704, :] = jnp.zeros((64, LENGTH), bf16)

    for e in range(2):
        for src in range(HEADS):
            for i in range(8):
                at = (src * 8 + i) * GROUP
                for parity in range(2):
                    lane = i * 2 * KW + parity * (KW - 64)
                    q_all[e, parity, at : at + GROUP, :] = q_ref[src, e, :, lane : lane + 640]
                lane = MAIN_LANES + i * DI
                qi_all[e, at : at + GROUP, :] = q_ref[src, e, :, lane : lane + DI]
                lane = MAIN_LANES + INDEX_LANES
                column = q_ref[src, e, :, lane : lane + 128].astype(f32)[:, i : i + 1]
                w_all[e, at : at + GROUP, :] = jnp.broadcast_to(column, (GROUP, DI))

    take = lax.broadcasted_iota(jnp.int32, (256, 256), 0)
    give = lax.broadcasted_iota(jnp.int32, (256, 256), 1)
    source = jnp.where(give // 64 == 1, give + 64, jnp.where(give // 64 == 2, give - 64, give))
    shuffle = jnp.where(take == source, 1.0, 0.0).astype(bf16)

    def sort_pair(i, carry):
        arrived(2 * i)
        arrived(2 * i + 1)
        both = jnp.concatenate([raw[2 * i], raw[2 * i + 1]], axis=1)
        mixed = jnp.dot(both, shuffle, preferred_element_type=f32).astype(bf16)
        early = pl.multiple_of(i * 128, 128)
        late = pl.multiple_of(HALF + i * 128, 128)
        keys[64:640, pl.ds(early, 128)] = mixed[0:KW, 0:128]
        keys[704:832, pl.ds(early, 128)] = mixed[KW:, 0:128]
        keys[64:640, pl.ds(late, 128)] = mixed[0:KW, 128:256]
        keys[704:832, pl.ds(late, 128)] = mixed[KW:, 128:256]
        return carry

    lax.fori_loop(0, 16, sort_pair, 0)

    key_grad[...] = jnp.zeros((DI, LENGTH), f32)

    for e in range(2):
        row_pos = lax.broadcasted_iota(jnp.int32, (GROUP, 1), 0) + h_own * GROUP
        row_pos = row_pos + (c_own if e == 0 else 63 - c_own) * BLOCK

        def key_pos(at, width):
            lane = lax.broadcasted_iota(jnp.int32, (1, width), 1) + at
            late_lane = lane - HALF
            late_pos = (63 - late_lane // BLOCK) * BLOCK + late_lane % BLOCK
            return jnp.where(lane < HALF, lane, late_pos)

        early_tiles = c_own // 4 + 1 if e == 0 else TILES // 2
        late_tiles = 0 if e == 0 else TILES // 2 - c_own // 4

        def tile_at(j):
            if e == 0:
                return pl.multiple_of(j * TILE, TILE)
            return pl.multiple_of(jnp.where(j < TILES // 2, j, j + c_own // 4) * TILE, TILE)

        steps = early_tiles + late_tiles

        best[...] = jnp.full((ROWS, 128), masked_value, f32)
        total[...] = jnp.zeros((ROWS, 128), f32)
        target[...] = jnp.zeros((GROUP, LENGTH), f32)
        logits[...] = jnp.full((GROUP, LENGTH), masked_value, f32)

        def score_step(j, carry):
            at = tile_at(j)
            visible = key_pos(at, TILE) <= row_pos
            for parity in range(2):
                k = keys[64 * (1 - parity) : 64 * (1 - parity) + 640, pl.ds(at, TILE)]
                s = jnp.dot(q_all[e, parity], k, preferred_element_type=f32)
                s = jnp.where(visible[None], s.reshape(HM // 2, GROUP, TILE), masked_value)
                s = s.reshape(ROWS // 2, TILE)
                r = slice(parity * (ROWS // 2), (parity + 1) * (ROWS // 2))
                scores[r, pl.ds(at, TILE)] = s
                best[r] = jnp.maximum(best[r], jnp.maximum(s[:, 0:128], s[:, 128:256]))
            return carry

        lax.fori_loop(0, steps, score_step, 0)

        def top_step(g, carry):
            r = pl.ds(pl.multiple_of(g * 128, 128), 128)
            best[r] = jnp.broadcast_to(jnp.max(best[r], axis=1, keepdims=True), (128, 128))
            return carry

        lax.fori_loop(0, ROWS // 128, top_step, 0)

        def exp_step(j, carry):
            at = tile_at(j)
            for g in range(ROWS // 128):
                r = slice(g * 128, (g + 1) * 128)
                top = best[r]
                part = total[r]
                for half in range(TILE // 128):
                    lanes = pl.ds(pl.multiple_of(at + half * 128, 128), 128)
                    raised = jnp.exp2((scores[r, lanes] - top) * SCORE_EXP2)
                    scores[r, lanes] = raised
                    part = part + raised
                total[r] = part
            return carry

        lax.fori_loop(0, steps, exp_step, 0)

        def total_step(g, carry):
            r = pl.ds(pl.multiple_of(g * 128, 128), 128)
            whole = jnp.sum(total[r], axis=1, keepdims=True)
            total[r] = jnp.broadcast_to((1.0 / HM) / whole, (128, 128))
            return carry

        lax.fori_loop(0, ROWS // 128, total_step, 0)

        def index_logits(at):
            act = jnp.dot(
                qi_all[e], keys[704:832, pl.ds(at, TILE)], preferred_element_type=f32
            )
            out = jnp.zeros((GROUP, TILE), f32)
            for h in range(HI):
                r = slice(h * GROUP, (h + 1) * GROUP)
                w = w_all[e, r]
                out = out + jnp.maximum(act[r], 0.0) * jnp.concatenate([w, w], axis=1)
            return out

        def target_step(j, carry):
            at = tile_at(j)
            lanes = pl.ds(at, TILE)
            acc = jnp.zeros((GROUP, TILE), f32)
            for h in range(HM):
                r = slice(h * GROUP, (h + 1) * GROUP)
                share = total[r]
                acc = acc + scores[r, lanes] * jnp.concatenate([share, share], axis=1)
            target[:, lanes] = acc
            visible = key_pos(at, TILE) <= row_pos
            logits[:, lanes] = jnp.where(visible, index_logits(at), masked_value)
            return carry

        lax.fori_loop(0, steps, target_step, 0)

        masked = logits[...]
        visible = masked > 0.5 * masked_value
        top_logit = jnp.max(masked, axis=1, keepdims=True)
        lse = top_logit + jnp.log(jnp.sum(jnp.exp(masked - top_logit), axis=1, keepdims=True))
        loss = jnp.sum(jnp.where(visible, target[...] * (lse - masked), 0.0), axis=1, keepdims=True)
        rounded = jnp.where(visible, jnp.exp(masked - lse) - target[...], 0.0).astype(bf16)
        slope[...] = rounded.astype(f32)

        gsum[...] = jnp.zeros((IROWS, DI), f32)
        q_float = qi_all[e].astype(f32)
        weighted = jnp.transpose(q_float * w_all[e]).astype(bf16)

        def back_step(j, carry):
            at = tile_at(j)
            lanes = pl.ds(at, TILE)
            k = keys[704:832, lanes]
            act = jnp.dot(qi_all[e], k, preferred_element_type=f32)
            through = jnp.where(
                act.reshape(HI, GROUP, TILE) > 0.0, slope[:, lanes][None], 0.0
            ).reshape(IROWS, TILE).astype(bf16)
            gsum[...] += nt_dot(through, k)
            key_grad[:, lanes] += jnp.dot(weighted, through, preferred_element_type=f32)
            return carry

        lax.fori_loop(0, steps, back_step, 0)

        grads = (gsum[...] * w_all[e]).astype(bf16)
        column = jnp.sum(gsum[...] * q_float, axis=1, keepdims=True)
        lane = lax.broadcasted_iota(jnp.int32, (GROUP, 128), 1)
        high = loss.astype(bf16).astype(f32)
        middle = (loss - high).astype(bf16).astype(f32)
        low = loss - high - middle
        extra = jnp.where(lane == 8, high, jnp.where(lane == 9, middle, jnp.where(lane == 10, low, 0.0)))
        for dst in range(HEADS):
            small = extra
            for i in range(8):
                at = (dst * 8 + i) * GROUP
                to = KEY_ROWS + (e * 9 + i) * GROUP
                out_ref[dst, to : to + GROUP, :] = grads[at : at + GROUP]
                small = jnp.where(lane == i, column[at : at + GROUP], small)
            to = KEY_ROWS + (e * 9 + 8) * GROUP
            out_ref[dst, to : to + GROUP, :] = small.astype(bf16)

    def emit(i, carry):
        for late in range(2):
            lanes = pl.ds(pl.multiple_of(late * HALF + i * 128, 128), 128)
            turned = jnp.transpose(key_grad[:, lanes]).astype(bf16)
            for k in range(4):
                to = pl.multiple_of(i * 64 + (k // 2) * 32, 32)
                out_ref[2 * late + k % 2, pl.ds(to, 32), :] = turned[k * 32 : (k + 1) * 32]
        return carry

    lax.fori_loop(0, 16, emit, 0)


def rows_call(slots, meta, pieces, queries):
    return pl.pallas_call(
        rows_kernel,
        out_shape=jax.ShapeDtypeStruct((HEADS, KEY_ROWS + GRAD_ROWS, DI), bf16),
        in_specs=[
            pl.BlockSpec(memory_space=pltpu.SMEM),
            pl.BlockSpec(memory_space=pltpu.SMEM),
            *[pl.BlockSpec(memory_space=pl.ANY)] * (2 * PIECES),
            pl.BlockSpec(memory_space=pltpu.VMEM),
        ],
        out_specs=pl.BlockSpec(memory_space=pltpu.VMEM),
        scratch_shapes=[
            pltpu.VMEM((32, KW + DI, 128), bf16),
            pltpu.VMEM((832, LENGTH), bf16),
            pltpu.VMEM((2, 2, ROWS // 2, 640), bf16),
            pltpu.VMEM((2, IROWS, DI), bf16),
            pltpu.VMEM((ROWS, LENGTH), f32),
            pltpu.VMEM((ROWS, 128), f32),
            pltpu.VMEM((ROWS, 128), f32),
            pltpu.VMEM((2, IROWS, DI), f32),
            pltpu.VMEM((GROUP, LENGTH), f32),
            pltpu.VMEM((GROUP, LENGTH), f32),
            pltpu.VMEM((GROUP, LENGTH), f32),
            pltpu.VMEM((IROWS, DI), f32),
            pltpu.VMEM((DI, LENGTH), f32),
            pltpu.SemaphoreType.DMA((32,)),
        ],
        compiler_params=pltpu.CompilerParams(vmem_limit_bytes=58 * 1024 * 1024),
        name="rows_work",
    )(slots, meta, *pieces, queries)


def spread_kernel(to_ref, got_ref, out_ref, sums):
    total = got_ref[0, 0:KEY_ROWS].astype(f32)
    for src in range(1, HEADS):
        total = total + got_ref[src, 0:KEY_ROWS].astype(f32)
    sums[0:KEY_ROWS] = total.astype(bf16)
    sums[KEY_ROWS:] = jnp.zeros((32, DI), bf16)

    def put(d, carry):
        out_ref[d] = sums[pl.ds(pl.multiple_of(to_ref[d] * 32, 32), 32)]
        return carry

    lax.fori_loop(0, 64, put, 0, unroll=8)


def spread_call(to, got):
    return pl.pallas_call(
        spread_kernel,
        out_shape=jax.ShapeDtypeStruct((64, 32, DI), bf16),
        in_specs=[
            pl.BlockSpec(memory_space=pltpu.SMEM),
            pl.BlockSpec(memory_space=pltpu.VMEM),
        ],
        out_specs=pl.BlockSpec(memory_space=pltpu.VMEM),
        scratch_shapes=[pltpu.VMEM((KEY_ROWS + 32, DI), bf16)],
        name="spread_keys",
    )(to, got)


def body(block_order, main_query, latent_key, index_query, index_weight, index_key):
    d_own = lax.axis_index(CTX)
    early = block_order.reshape(64, 2)[:, 0]
    own = lax.dynamic_index_in_dim(early, d_own, 0, keepdims=False)
    first = own // 64 * 64
    c_own = own - first
    in_order = jnp.where(early // 64 * 64 == first, early - first, -1).reshape(4, 8, 2)
    for axis in range(3):
        own_at = lax.axis_index(CTX[axis])
        order = (lax.iota(jnp.int32, in_order.shape[axis]) + own_at) % in_order.shape[axis]
        in_order = jnp.take(in_order, order, axis=axis)
    slots = in_order.reshape(64)
    to = jnp.where(early // 64 * 64 == first, early - first, 32)
    meta = jnp.stack([c_own, lax.axis_index("head"), lax.axis_index("ctx_2")]).astype(jnp.int32)

    shard = jnp.concatenate([latent_key, index_key], axis=0)
    pieces = gather_keys(shard)

    weights = jnp.pad(index_weight, ((0, 0), (0, 128 - index_weight.shape[1])))
    rows = jnp.concatenate([main_query, index_query.reshape(128, INDEX_LANES), weights], axis=1)
    rows = rows.reshape(2, HEADS, GROUP, ALL_LANES).swapaxes(0, 1)
    queries = lax.all_to_all(rows, "head", split_axis=0, concat_axis=0, tiled=True)

    sent = rows_call(slots, meta, pieces, queries)
    got = lax.all_to_all(sent, "head", split_axis=0, concat_axis=0, tiled=True)
    parts = lax.all_to_all(spread_call(to, got), CTX, split_axis=0, concat_axis=0, tiled=True)
    grad_key = jnp.sum(parts.astype(f32), axis=0)

    grads = got[:, KEY_ROWS:].reshape(HEADS, 2, 9, GROUP, DI).transpose(1, 0, 3, 2, 4)
    grads = grads.reshape(128, 9, DI)
    small = grads[:, 8]
    row_loss = jnp.sum(small[:, 8:11].astype(f32), axis=1)
    return (row_loss, grads[:, 0:8], small[:, 0:8], grad_key)


def onward(piece, axis):
    n = lax.axis_size(axis)
    return lax.ppermute(piece, axis, [(i, (i + 1) % n) for i in range(n)])


def backward(piece, axis):
    n = lax.axis_size(axis)
    return lax.ppermute(piece, axis, [(i, (i - 1) % n) for i in range(n)])


def swapped(piece):
    return lax.ppermute(piece, "ctx_2", [(0, 1), (1, 0)])


def gather_keys(shard):
    core = lax.axis_index("ctx_2")
    top, bottom = shard[:HALF_ROWS], shard[HALF_ROWS:]
    mine = jnp.where(core == 0, top, bottom)
    given = jnp.where(core == 0, bottom, top)
    block = jnp.stack([mine, swapped(given)])
    first, second = block[:, :STRIP], block[:, STRIP:]

    z, y = "ctx_1", "ctx_0"
    u1, d1 = onward(first, z), backward(first, z)
    g1, h1 = onward(second, y), backward(second, y)
    u2, d2 = onward(u1, z), backward(d1, z)
    g2 = onward(g1, y)
    u3, d3 = onward(u2, z), backward(d2, z)
    rows = jnp.stack([second, h1, g2, g1])
    u4 = onward(u3, z)
    planes = jnp.stack([first, d1, d2, d3, u4, u3, u2, u1])

    up1, down1 = onward(planes, y), backward(planes, y)
    up2, down2 = onward(up1[:4], y), backward(down1[4:], y)
    b1, f1 = backward(rows, z), onward(rows, z)
    b2, f2 = backward(b1, z), onward(f1, z)
    b3, f3 = backward(b2, z), onward(f2, z)
    f4, b4 = onward(f3[:2], z), backward(b3[2:], z)
    own = [planes, down1, up1, up2, down2, rows, b1, b2, b3, f3, f2, f1, f4, b4]
    return own + [swapped(piece) for piece in own]


def solution(mesh):
    split = Mesh(
        mesh.devices.reshape(4, 8, 2, mesh.shape["head"]), ("ctx_0", "ctx_1", "ctx_2", "head")
    )
    in_specs = (
        P(),
        P(CTX, "head"),
        P(None, CTX),
        P(CTX, "head", None),
        P(CTX, "head"),
        P(None, CTX),
    )
    out_specs = (P(CTX), P(CTX, "head", None), P(CTX, "head"), P(CTX_HEAD, None))
    return jax.shard_map(body, mesh=split, in_specs=in_specs, out_specs=out_specs, check_vma=False)
```

```python
import math

import jax
import jax.numpy as jnp
from jax import lax
from jax.experimental import pallas as pl
from jax.experimental.pallas import tpu as pltpu
from jax.sharding import Mesh
from jax.sharding import PartitionSpec as P

HM = 64
HI = 32
DI = 128
KW = 576
HEAD_QK = 192
BLOCK = 64
LENGTH = 4096
HALF = LENGTH // 2
CTX = ("ctx_0", "ctx_1", "ctx_2")
CTX_HEAD = ("ctx_0", "ctx_1", "ctx_2", "head")
HEADS = 4
GROUP = 16
MAIN_LANES = HM // HEADS * KW
INDEX_LANES = HI // HEADS * DI
ALL_LANES = MAIN_LANES + INDEX_LANES + 128
TILE = 256
TILES = LENGTH // TILE
PAIRS = LENGTH // TILE
ROWS = HM * GROUP
IROWS = HI * GROUP
KEY_ROWS = 1024
GRAD_ROWS = 9 * 2 * GROUP
HALF_ROWS = (KW + DI) // 2
STRIP = HALF_ROWS // 2
PIECES = 14
masked_value = -1e30
SCORE_EXP2 = math.log2(math.e) / math.sqrt(HEAD_QK)
f32 = jnp.float32
bf16 = jnp.bfloat16


def sources(y, z):
    if y == 2:
        a = (3, z) if z < 4 else (4, z - 4)
    else:
        a = ({0: 0, 1: 1, 3: 2}[y], z)
    if z == 4:
        b = (12, y) if y < 2 else (13, y - 2)
    else:
        b = ({0: 5, 1: 6, 2: 7, 3: 8, 5: 9, 6: 10, 7: 11}[z], y)
    return a, b


def nt_dot(a, b):
    return lax.dot_general(a, b, (((1,), (1,)), ((), ())), preferred_element_type=f32)


def own_block(order_ref):
    y, z, core = (lax.axis_index(axis) for axis in CTX)
    own = order_ref[((y * 8 + z) * 2 + core) * 2]
    first = jnp.where(own >= 64, 64, 0)
    return first, own - first


def rows_kernel(order_ref, *refs):
    pieces = refs[: 2 * PIECES]
    q_ref, out_ref = refs[2 * PIECES : 2 * PIECES + 2]
    (
        raw, keys, q_all, qi_all, scores, best, total, w_all, target, logits, slope, gsum,
        key_grad, sems,
    ) = refs[2 * PIECES + 2 :]
    y_own, z_own, core_own = (lax.axis_index(axis) for axis in CTX)
    h_own = lax.axis_index("head")
    first, c_own = own_block(order_ref)
    own_half = pl.multiple_of(core_own * HALF_ROWS, 16)
    other_half = pl.multiple_of((1 - core_own) * HALF_ROWS, 16)

    for y in range(4):
        for z in range(8):
            for core in range(2):
                place = ((y_own + y) % 4 * 8 + (z_own + z) % 8) * 2 + (core_own + core) % 2
                slot = order_ref[2 * place] - first

                @pl.when((slot >= 0) & (slot < 64))
                def _():
                    for (piece, block), at in zip(sources(y, z), (0, STRIP)):
                        for kind, half in ((0, own_half), (1, other_half)):
                            pltpu.make_async_copy(
                                pieces[kind * PIECES + piece].at[block, core ^ kind],
                                raw.at[slot, pl.ds(half + at, STRIP), :],
                                sems.at[slot],
                            ).start()

    def arrived(n):
        pltpu.make_async_copy(raw.at[n], raw.at[n], sems.at[n]).wait()

    keys[0:64, :] = jnp.zeros((64, LENGTH), bf16)
    keys[640:704, :] = jnp.zeros((64, LENGTH), bf16)

    for e in range(2):
        for src in range(HEADS):
            for i in range(8):
                at = (src * 8 + i) * GROUP
                for parity in range(2):
                    lane = i * 2 * KW + parity * (KW - 64)
                    q_all[e, parity, at : at + GROUP, :] = q_ref[src, e, :, lane : lane + 640]
                lane = MAIN_LANES + i * DI
                qi_all[e, at : at + GROUP, :] = q_ref[src, e, :, lane : lane + DI]
                lane = MAIN_LANES + INDEX_LANES
                column = q_ref[src, e, :, lane : lane + 128].astype(f32)[:, i : i + 1]
                w_all[e, at : at + GROUP, :] = jnp.broadcast_to(column, (GROUP, DI))

    take = lax.broadcasted_iota(jnp.int32, (256, 256), 0)
    give = lax.broadcasted_iota(jnp.int32, (256, 256), 1)
    source = jnp.where(give // 64 == 1, give + 64, jnp.where(give // 64 == 2, give - 64, give))
    shuffle = jnp.where(take == source, 1.0, 0.0).astype(bf16)

    def sort_pair(i, carry):
        arrived(2 * i)
        arrived(2 * i + 1)
        both = jnp.concatenate([raw[2 * i], raw[2 * i + 1]], axis=1)
        mixed = jnp.dot(both, shuffle, preferred_element_type=f32).astype(bf16)
        early = pl.multiple_of(i * 128, 128)
        late = pl.multiple_of(HALF + i * 128, 128)
        keys[64:640, pl.ds(early, 128)] = mixed[0:KW, 0:128]
        keys[704:832, pl.ds(early, 128)] = mixed[KW:, 0:128]
        keys[64:640, pl.ds(late, 128)] = mixed[0:KW, 128:256]
        keys[704:832, pl.ds(late, 128)] = mixed[KW:, 128:256]
        return carry

    lax.fori_loop(0, 16, sort_pair, 0)

    key_grad[...] = jnp.zeros((DI, LENGTH), f32)

    for e in range(2):
        row_pos = lax.broadcasted_iota(jnp.int32, (GROUP, 1), 0) + h_own * GROUP
        row_pos = row_pos + (c_own if e == 0 else 63 - c_own) * BLOCK

        def key_pos(at, width):
            lane = lax.broadcasted_iota(jnp.int32, (1, width), 1) + at
            late_lane = lane - HALF
            late_pos = (63 - late_lane // BLOCK) * BLOCK + late_lane % BLOCK
            return jnp.where(lane < HALF, lane, late_pos)

        early_tiles = c_own // 4 + 1 if e == 0 else TILES // 2
        late_tiles = 0 if e == 0 else TILES // 2 - c_own // 4

        def tile_at(j):
            if e == 0:
                return pl.multiple_of(j * TILE, TILE)
            return pl.multiple_of(jnp.where(j < TILES // 2, j, j + c_own // 4) * TILE, TILE)

        steps = early_tiles + late_tiles

        best[...] = jnp.full((ROWS, 128), masked_value, f32)
        total[...] = jnp.zeros((ROWS, 128), f32)
        target[...] = jnp.zeros((GROUP, LENGTH), f32)
        logits[...] = jnp.full((GROUP, LENGTH), masked_value, f32)

        def score_step(j, carry):
            at = tile_at(j)
            visible = key_pos(at, TILE) <= row_pos
            for parity in range(2):
                k = keys[64 * (1 - parity) : 64 * (1 - parity) + 640, pl.ds(at, TILE)]
                s = jnp.dot(q_all[e, parity], k, preferred_element_type=f32)
                s = jnp.where(visible[None], s.reshape(HM // 2, GROUP, TILE), masked_value)
                s = s.reshape(ROWS // 2, TILE)
                r = slice(parity * (ROWS // 2), (parity + 1) * (ROWS // 2))
                scores[r, pl.ds(at, TILE)] = s
                best[r] = jnp.maximum(best[r], jnp.maximum(s[:, 0:128], s[:, 128:256]))
            return carry

        lax.fori_loop(0, steps, score_step, 0)

        def top_step(g, carry):
            r = pl.ds(pl.multiple_of(g * 128, 128), 128)
            best[r] = jnp.broadcast_to(jnp.max(best[r], axis=1, keepdims=True), (128, 128))
            return carry

        lax.fori_loop(0, ROWS // 128, top_step, 0)

        def exp_step(j, carry):
            at = tile_at(j)
            for g in range(ROWS // 128):
                r = slice(g * 128, (g + 1) * 128)
                top = best[r]
                part = total[r]
                for half in range(TILE // 128):
                    lanes = pl.ds(pl.multiple_of(at + half * 128, 128), 128)
                    raised = jnp.exp2((scores[r, lanes] - top) * SCORE_EXP2)
                    scores[r, lanes] = raised
                    part = part + raised
                total[r] = part
            return carry

        lax.fori_loop(0, steps, exp_step, 0)

        def total_step(g, carry):
            r = pl.ds(pl.multiple_of(g * 128, 128), 128)
            whole = jnp.sum(total[r], axis=1, keepdims=True)
            total[r] = jnp.broadcast_to((1.0 / HM) / whole, (128, 128))
            return carry

        lax.fori_loop(0, ROWS // 128, total_step, 0)

        def index_logits(at):
            act = jnp.dot(
                qi_all[e], keys[704:832, pl.ds(at, TILE)], preferred_element_type=f32
            )
            out = jnp.zeros((GROUP, TILE), f32)
            for h in range(HI):
                r = slice(h * GROUP, (h + 1) * GROUP)
                w = w_all[e, r]
                out = out + jnp.maximum(act[r], 0.0) * jnp.concatenate([w, w], axis=1)
            return out

        def target_step(j, carry):
            at = tile_at(j)
            lanes = pl.ds(at, TILE)
            acc = jnp.zeros((GROUP, TILE), f32)
            for h in range(HM):
                r = slice(h * GROUP, (h + 1) * GROUP)
                share = total[r]
                acc = acc + scores[r, lanes] * jnp.concatenate([share, share], axis=1)
            target[:, lanes] = acc
            visible = key_pos(at, TILE) <= row_pos
            logits[:, lanes] = jnp.where(visible, index_logits(at), masked_value)
            return carry

        lax.fori_loop(0, steps, target_step, 0)

        masked = logits[...]
        visible = masked > 0.5 * masked_value
        top_logit = jnp.max(masked, axis=1, keepdims=True)
        lse = top_logit + jnp.log(jnp.sum(jnp.exp(masked - top_logit), axis=1, keepdims=True))
        loss = jnp.sum(jnp.where(visible, target[...] * (lse - masked), 0.0), axis=1, keepdims=True)
        rounded = jnp.where(visible, jnp.exp(masked - lse) - target[...], 0.0).astype(bf16)
        slope[...] = rounded.astype(f32)

        gsum[...] = jnp.zeros((IROWS, DI), f32)
        q_float = qi_all[e].astype(f32)
        weighted = jnp.transpose(q_float * w_all[e]).astype(bf16)

        def back_step(j, carry):
            at = tile_at(j)
            lanes = pl.ds(at, TILE)
            k = keys[704:832, lanes]
            act = jnp.dot(qi_all[e], k, preferred_element_type=f32)
            through = jnp.where(
                act.reshape(HI, GROUP, TILE) > 0.0, slope[:, lanes][None], 0.0
            ).reshape(IROWS, TILE).astype(bf16)
            gsum[...] += nt_dot(through, k)
            key_grad[:, lanes] += jnp.dot(weighted, through, preferred_element_type=f32)
            return carry

        lax.fori_loop(0, steps, back_step, 0)

        grads = (gsum[...] * w_all[e]).astype(bf16)
        column = jnp.sum(gsum[...] * q_float, axis=1, keepdims=True)
        lane = lax.broadcasted_iota(jnp.int32, (GROUP, 128), 1)
        high = loss.astype(bf16).astype(f32)
        middle = (loss - high).astype(bf16).astype(f32)
        low = loss - high - middle
        extra = jnp.where(lane == 8, high, jnp.where(lane == 9, middle, jnp.where(lane == 10, low, 0.0)))
        for dst in range(HEADS):
            small = extra
            for i in range(8):
                at = (dst * 8 + i) * GROUP
                to = KEY_ROWS + (e * 9 + i) * GROUP
                out_ref[dst, to : to + GROUP, :] = grads[at : at + GROUP]
                small = jnp.where(lane == i, column[at : at + GROUP], small)
            to = KEY_ROWS + (e * 9 + 8) * GROUP
            out_ref[dst, to : to + GROUP, :] = small.astype(bf16)

    def emit(i, carry):
        for late in range(2):
            lanes = pl.ds(pl.multiple_of(late * HALF + i * 128, 128), 128)
            turned = jnp.transpose(key_grad[:, lanes]).astype(bf16)
            for k in range(4):
                to = pl.multiple_of(i * 64 + (k // 2) * 32, 32)
                out_ref[2 * late + k % 2, pl.ds(to, 32), :] = turned[k * 32 : (k + 1) * 32]
        return carry

    lax.fori_loop(0, 16, emit, 0)


def rows_call(order, pieces, queries):
    return pl.pallas_call(
        rows_kernel,
        out_shape=jax.ShapeDtypeStruct((HEADS, KEY_ROWS + GRAD_ROWS, DI), bf16),
        in_specs=[
            pl.BlockSpec(memory_space=pltpu.SMEM),
            *[pl.BlockSpec(memory_space=pl.ANY)] * (2 * PIECES),
            pl.BlockSpec(memory_space=pltpu.VMEM),
        ],
        out_specs=pl.BlockSpec(memory_space=pltpu.VMEM),
        scratch_shapes=[
            pltpu.VMEM((32, KW + DI, 128), bf16),
            pltpu.VMEM((832, LENGTH), bf16),
            pltpu.VMEM((2, 2, ROWS // 2, 640), bf16),
            pltpu.VMEM((2, IROWS, DI), bf16),
            pltpu.VMEM((ROWS, LENGTH), f32),
            pltpu.VMEM((ROWS, 128), f32),
            pltpu.VMEM((ROWS, 128), f32),
            pltpu.VMEM((2, IROWS, DI), f32),
            pltpu.VMEM((GROUP, LENGTH), f32),
            pltpu.VMEM((GROUP, LENGTH), f32),
            pltpu.VMEM((GROUP, LENGTH), f32),
            pltpu.VMEM((IROWS, DI), f32),
            pltpu.VMEM((DI, LENGTH), f32),
            pltpu.SemaphoreType.DMA((32,)),
        ],
        compiler_params=pltpu.CompilerParams(vmem_limit_bytes=58 * 1024 * 1024),
        name="rows_work",
    )(order, *pieces, queries)


def spread_kernel(order_ref, got_ref, out_ref, sums):
    first, c_own = own_block(order_ref)
    total = got_ref[0, 0:KEY_ROWS].astype(f32)
    for src in range(1, HEADS):
        total = total + got_ref[src, 0:KEY_ROWS].astype(f32)
    sums[0:KEY_ROWS] = total.astype(bf16)
    sums[KEY_ROWS:] = jnp.zeros((32, DI), bf16)

    def put(d, carry):
        slot = order_ref[2 * d] - first
        slot = jnp.where((slot >= 0) & (slot < 64), slot, 32)
        out_ref[d] = sums[pl.ds(pl.multiple_of(slot * 32, 32), 32)]
        return carry

    lax.fori_loop(0, 64, put, 0, unroll=8)


def spread_call(order, got):
    return pl.pallas_call(
        spread_kernel,
        out_shape=jax.ShapeDtypeStruct((64, 32, DI), bf16),
        in_specs=[
            pl.BlockSpec(memory_space=pltpu.SMEM),
            pl.BlockSpec(memory_space=pltpu.VMEM),
        ],
        out_specs=pl.BlockSpec(memory_space=pltpu.VMEM),
        scratch_shapes=[pltpu.VMEM((KEY_ROWS + 32, DI), bf16)],
        name="spread_keys",
    )(order, got)


def body(block_order, main_query, latent_key, index_query, index_weight, index_key):
    shard = jnp.concatenate([latent_key, index_key], axis=0)
    pieces, started = gather_keys(shard)

    weights = jnp.pad(index_weight, ((0, 0), (0, 128 - index_weight.shape[1])))
    rows = jnp.concatenate([main_query, index_query.reshape(128, INDEX_LANES), weights], axis=1)
    rows = rows.reshape(2, HEADS, GROUP, ALL_LANES).swapaxes(0, 1)
    rows, _ = lax.optimization_barrier((rows, started))
    queries = lax.all_to_all(rows, "head", split_axis=0, concat_axis=0, tiled=True)

    sent = rows_call(block_order, pieces, queries)
    got = lax.all_to_all(sent, "head", split_axis=0, concat_axis=0, tiled=True)
    parts = lax.all_to_all(spread_call(block_order, got), CTX, split_axis=0, concat_axis=0, tiled=True)
    grad_key = jnp.sum(parts.astype(f32), axis=0)

    grads = got[:, KEY_ROWS:].reshape(HEADS, 2, 9, GROUP, DI).transpose(1, 0, 3, 2, 4)
    grads = grads.reshape(128, 9, DI)
    small = grads[:, 8]
    row_loss = jnp.sum(small[:, 8:11].astype(f32), axis=1)
    return (row_loss, grads[:, 0:8], small[:, 0:8], grad_key)


def onward(piece, axis):
    n = lax.axis_size(axis)
    return lax.ppermute(piece, axis, [(i, (i + 1) % n) for i in range(n)])


def backward(piece, axis):
    n = lax.axis_size(axis)
    return lax.ppermute(piece, axis, [(i, (i - 1) % n) for i in range(n)])


def swapped(piece):
    return lax.ppermute(piece, "ctx_2", [(0, 1), (1, 0)])


def gather_keys(shard):
    core = lax.axis_index("ctx_2")
    top, bottom = shard[:HALF_ROWS], shard[HALF_ROWS:]
    mine = jnp.where(core == 0, top, bottom)
    given = jnp.where(core == 0, bottom, top)
    block = jnp.stack([mine, swapped(given)])
    first, second = block[:, :STRIP], block[:, STRIP:]

    z, y = "ctx_1", "ctx_0"
    u1, d1 = onward(first, z), backward(first, z)
    g1, h1 = onward(second, y), backward(second, y)
    u2, d2 = onward(u1, z), backward(d1, z)
    g2 = onward(g1, y)
    u3, d3 = onward(u2, z), backward(d2, z)
    u4 = onward(u3, z)
    rows = jnp.stack([second, h1, g2, g1])
    rows, u3, d3 = lax.optimization_barrier((rows, u3, d3))
    planes = jnp.stack([first, d1, d2, d3, u4, u3, u2, u1])

    up1, down1 = onward(planes, y), backward(planes, y)
    up2, down2 = onward(up1[:4], y), backward(down1[4:], y)
    b1, f1 = backward(rows, z), onward(rows, z)
    b2, f2 = backward(b1, z), onward(f1, z)
    b3, f3 = backward(b2, z), onward(f2, z)
    f4, b4 = onward(f3[:2], z), backward(b3[2:], z)
    own = [planes, down1, up1, up2, down2, rows, b1, b2, b3, f3, f2, f1, f4, b4]
    return own + [swapped(piece) for piece in own], u4


def solution(mesh):
    split = Mesh(
        mesh.devices.reshape(4, 8, 2, mesh.shape["head"]), ("ctx_0", "ctx_1", "ctx_2", "head")
    )
    in_specs = (
        P(),
        P(CTX, "head"),
        P(None, CTX),
        P(CTX, "head", None),
        P(CTX, "head"),
        P(None, CTX),
    )
    out_specs = (P(CTX), P(CTX, "head", None), P(CTX, "head"), P(CTX_HEAD, None))
    return jax.shard_map(body, mesh=split, in_specs=in_specs, out_specs=out_specs, check_vma=False)
```

```python
import math

import jax
import jax.numpy as jnp
from jax import lax
from jax.experimental import pallas as pl
from jax.experimental.pallas import tpu as pltpu
from jax.sharding import Mesh
from jax.sharding import PartitionSpec as P


HM = 64
HI = 32
DI = 128
KW = 576
HEAD_QK = 192
BLOCK = 64
LENGTH = 4096
HALF = LENGTH // 2
CTX = ("ctx_0", "ctx_1", "ctx_2")
CTX_HEAD = ("ctx_0", "ctx_1", "ctx_2", "head")
HEADS = 4
GROUP = 16
MAIN_LANES = HM // HEADS * KW
INDEX_LANES = HI // HEADS * DI
ALL_LANES = MAIN_LANES + INDEX_LANES + 128
TILE = 256
TILES = LENGTH // TILE
WIDE = 512
ROWS = HM * GROUP
IROWS = HI * GROUP
KEY_ROWS = 1024
GRAD_ROWS = 9 * 2 * GROUP
HALF_ROWS = (KW + DI) // 2
STRIP = 208
STRIP_CUT = 112
REST = HALF_ROWS - STRIP
REST_CUT = 80
PIECES = 14
masked_value = -1e30
SCORE_EXP2 = math.log2(math.e) / math.sqrt(HEAD_QK)
f32 = jnp.float32
bf16 = jnp.bfloat16


def sources(y, z):
    if y == 2:
        first = [(3, 0, STRIP_CUT), (4, STRIP_CUT, STRIP - STRIP_CUT)]
    else:
        first = [({0: 0, 1: 1, 3: 2}[y], 0, STRIP)]
    if z == 4:
        rest = [(12, STRIP, REST_CUT), (13, STRIP + REST_CUT, REST - REST_CUT)]
    else:
        rest = [({0: 5, 1: 6, 2: 7, 3: 8, 5: 9, 6: 10, 7: 11}[z], STRIP, REST)]
    return first, rest


def nt_dot(a, b):
    return lax.dot_general(a, b, (((1,), (1,)), ((), ())), preferred_element_type=f32)


def own_block(order_ref):
    y, z, core = (lax.axis_index(axis) for axis in CTX)
    own = order_ref[((y * 8 + z) * 2 + core) * 2]
    first = jnp.where(own >= 64, 64, 0)
    return first, own - first


def rows_kernel(order_ref, *refs):
    pieces = refs[: 2 * PIECES]
    q_ref, out_ref = refs[2 * PIECES : 2 * PIECES + 2]
    (
        raw, keys, q_all, qi_all, scores, best, total, w_all, target, logits, slope, gsum,
        key_grad, sems,
    ) = refs[2 * PIECES + 2 :]
    y_own, z_own, core_own = (lax.axis_index(axis) for axis in CTX)
    h_own = lax.axis_index("head")
    first, c_own = own_block(order_ref)
    own_half = pl.multiple_of(core_own * HALF_ROWS, 16)
    other_half = pl.multiple_of((1 - core_own) * HALF_ROWS, 16)

    for y in range(4):
        for z in range(8):
            for core in range(2):
                y_from, z_from = (y_own + y) % 4, (z_own + z) % 8
                place = (y_from * 8 + z_from) * 2 + (core_own + core) % 2
                slot = order_ref[2 * place] - first

                @pl.when((slot >= 0) & (slot < 64))
                def _():
                    for parts, block in zip(sources(y, z), (z_from, y)):
                        for piece, at, size in parts:
                            for kind, half in ((0, own_half), (1, other_half)):
                                pltpu.make_async_copy(
                                    pieces[kind * PIECES + piece].at[block, core ^ kind],
                                    raw.at[slot, pl.ds(half + at, size), :],
                                    sems.at[slot],
                                ).start()

    def arrived(n):
        pltpu.make_async_copy(raw.at[n], raw.at[n], sems.at[n]).wait()

    keys[0:64, :] = jnp.zeros((64, LENGTH), bf16)
    keys[640:704, :] = jnp.zeros((64, LENGTH), bf16)

    for e in range(2):
        for src in range(HEADS):
            for i in range(8):
                at = (src * 8 + i) * GROUP
                for parity in range(2):
                    lane = i * 2 * KW + parity * (KW - 64)
                    q_all[e, parity, at : at + GROUP, :] = q_ref[src, e, :, lane : lane + 640]
                lane = MAIN_LANES + i * DI
                qi_all[e, at : at + GROUP, :] = q_ref[src, e, :, lane : lane + DI]
                lane = MAIN_LANES + INDEX_LANES
                column = q_ref[src, e, :, lane : lane + 128].astype(f32)[:, i : i + 1]
                w_all[e, at : at + GROUP, :] = jnp.broadcast_to(column, (GROUP, DI))

    take = lax.broadcasted_iota(jnp.int32, (256, 256), 0)
    give = lax.broadcasted_iota(jnp.int32, (256, 256), 1)
    source = jnp.where(give // 64 == 1, give + 64, jnp.where(give // 64 == 2, give - 64, give))
    shuffle = jnp.where(take == source, 1.0, 0.0).astype(bf16)

    def sort_pair(i, carry):
        arrived(2 * i)
        arrived(2 * i + 1)
        both = jnp.concatenate([raw[2 * i], raw[2 * i + 1]], axis=1)
        mixed = jnp.dot(both, shuffle, preferred_element_type=f32).astype(bf16)
        early = pl.multiple_of(i * 128, 128)
        late = pl.multiple_of(HALF + i * 128, 128)
        keys[64:640, pl.ds(early, 128)] = mixed[0:KW, 0:128]
        keys[704:832, pl.ds(early, 128)] = mixed[KW:, 0:128]
        keys[64:640, pl.ds(late, 128)] = mixed[0:KW, 128:256]
        keys[704:832, pl.ds(late, 128)] = mixed[KW:, 128:256]
        return carry

    lax.fori_loop(0, 16, sort_pair, 0)

    key_grad[...] = jnp.zeros((DI, LENGTH), f32)

    for e in range(2):
        row_pos = lax.broadcasted_iota(jnp.int32, (GROUP, 1), 0) + h_own * GROUP
        row_pos = row_pos + (c_own if e == 0 else 63 - c_own) * BLOCK

        def key_pos(at, width):
            lane = lax.broadcasted_iota(jnp.int32, (1, width), 1) + at
            late_lane = lane - HALF
            late_pos = (63 - late_lane // BLOCK) * BLOCK + late_lane % BLOCK
            return jnp.where(lane < HALF, lane, late_pos)

        early_tiles = c_own // 4 + 1 if e == 0 else TILES // 2
        late_tiles = 0 if e == 0 else TILES // 2 - c_own // 4

        def tile_at(j):
            if e == 0:
                return pl.multiple_of(j * TILE, TILE)
            return pl.multiple_of(jnp.where(j < TILES // 2, j, j + c_own // 4) * TILE, TILE)

        steps = early_tiles + late_tiles

        best[...] = jnp.full((ROWS, 128), masked_value, f32)
        total[...] = jnp.zeros((ROWS, 128), f32)
        target[...] = jnp.zeros((GROUP, LENGTH), f32)
        logits[...] = jnp.full((GROUP, LENGTH), masked_value, f32)

        wide_steps = c_own // 8 + 1 if e == 0 else LENGTH // WIDE - c_own // 8

        def score_step(j, carry):
            at = j if e == 0 else jnp.where(j < HALF // WIDE, j, j + c_own // 8)
            at = pl.multiple_of(at * WIDE, WIDE)
            visible = key_pos(at, WIDE) <= row_pos
            for parity in range(2):
                k = keys[64 * (1 - parity) : 64 * (1 - parity) + 640, pl.ds(at, WIDE)]
                s = jnp.dot(q_all[e, parity], k, preferred_element_type=f32)
                s = jnp.where(visible[None], s.reshape(HM // 2, GROUP, WIDE), masked_value)
                s = s.reshape(ROWS // 2, WIDE)
                r = slice(parity * (ROWS // 2), (parity + 1) * (ROWS // 2))
                scores[r, pl.ds(at, WIDE)] = s
                top = jnp.maximum(s[:, 0:128], s[:, 128:256])
                best[r] = jnp.maximum(best[r], jnp.maximum(top, jnp.maximum(s[:, 256:384], s[:, 384:512])))
            return carry

        lax.fori_loop(0, wide_steps, score_step, 0)

        def top_step(g, carry):
            r = pl.ds(pl.multiple_of(g * 128, 128), 128)
            best[r] = jnp.broadcast_to(jnp.max(best[r], axis=1, keepdims=True), (128, 128))
            return carry

        lax.fori_loop(0, ROWS // 128, top_step, 0)

        def exp_step(j, carry):
            at = tile_at(j)
            for g in range(ROWS // 128):
                r = slice(g * 128, (g + 1) * 128)
                top = best[r]
                part = total[r]
                for half in range(TILE // 128):
                    lanes = pl.ds(pl.multiple_of(at + half * 128, 128), 128)
                    raised = jnp.exp2((scores[r, lanes] - top) * SCORE_EXP2)
                    scores[r, lanes] = raised
                    part = part + raised
                total[r] = part
            return carry

        lax.fori_loop(0, steps, exp_step, 0)

        def total_step(g, carry):
            r = pl.ds(pl.multiple_of(g * 128, 128), 128)
            whole = jnp.sum(total[r], axis=1, keepdims=True)
            total[r] = jnp.broadcast_to((1.0 / HM) / whole, (128, 128))
            return carry

        lax.fori_loop(0, ROWS // 128, total_step, 0)

        def index_logits(at):
            act = jnp.dot(
                qi_all[e], keys[704:832, pl.ds(at, TILE)], preferred_element_type=f32
            )
            out = jnp.zeros((GROUP, TILE), f32)
            for h in range(HI):
                r = slice(h * GROUP, (h + 1) * GROUP)
                w = w_all[e, r]
                out = out + jnp.maximum(act[r], 0.0) * jnp.concatenate([w, w], axis=1)
            return out

        def target_step(j, carry):
            at = tile_at(j)
            lanes = pl.ds(at, TILE)
            acc = jnp.zeros((GROUP, TILE), f32)
            for h in range(HM):
                r = slice(h * GROUP, (h + 1) * GROUP)
                share = total[r]
                acc = acc + scores[r, lanes] * jnp.concatenate([share, share], axis=1)
            target[:, lanes] = acc
            visible = key_pos(at, TILE) <= row_pos
            logits[:, lanes] = jnp.where(visible, index_logits(at), masked_value)
            return carry

        lax.fori_loop(0, steps, target_step, 0)

        masked = logits[...]
        visible = masked > 0.5 * masked_value
        top_logit = jnp.max(masked, axis=1, keepdims=True)
        lse = top_logit + jnp.log(jnp.sum(jnp.exp(masked - top_logit), axis=1, keepdims=True))
        loss = jnp.sum(jnp.where(visible, target[...] * (lse - masked), 0.0), axis=1, keepdims=True)
        rounded = jnp.where(visible, jnp.exp(masked - lse) - target[...], 0.0).astype(bf16)
        slope[...] = rounded.astype(f32)

        gsum[...] = jnp.zeros((IROWS, DI), f32)
        q_float = qi_all[e].astype(f32)
        weighted = jnp.transpose(q_float * w_all[e]).astype(bf16)

        def back_step(j, carry):
            at = j if e == 0 else jnp.where(j < HALF // WIDE, j, j + c_own // 8)
            lanes = pl.ds(pl.multiple_of(at * WIDE, WIDE), WIDE)
            k = keys[704:832, lanes]
            act = jnp.dot(qi_all[e], k, preferred_element_type=f32)
            through = jnp.where(
                act.reshape(HI, GROUP, WIDE) > 0.0, slope[:, lanes][None], 0.0
            ).reshape(IROWS, WIDE).astype(bf16)
            gsum[...] += nt_dot(through, k)
            key_grad[:, lanes] += jnp.dot(weighted, through, preferred_element_type=f32)
            return carry

        lax.fori_loop(0, wide_steps, back_step, 0)

        grads = (gsum[...] * w_all[e]).astype(bf16)
        column = jnp.sum(gsum[...] * q_float, axis=1, keepdims=True)
        lane = lax.broadcasted_iota(jnp.int32, (GROUP, 128), 1)
        high = loss.astype(bf16).astype(f32)
        middle = (loss - high).astype(bf16).astype(f32)
        low = loss - high - middle
        extra = jnp.where(lane == 8, high, jnp.where(lane == 9, middle, jnp.where(lane == 10, low, 0.0)))
        for dst in range(HEADS):
            small = extra
            for i in range(8):
                at = (dst * 8 + i) * GROUP
                to = KEY_ROWS + (e * 9 + i) * GROUP
                out_ref[dst, to : to + GROUP, :] = grads[at : at + GROUP]
                small = jnp.where(lane == i, column[at : at + GROUP], small)
            to = KEY_ROWS + (e * 9 + 8) * GROUP
            out_ref[dst, to : to + GROUP, :] = small.astype(bf16)

    def emit(i, carry):
        for late in range(2):
            lanes = pl.ds(pl.multiple_of(late * HALF + i * 128, 128), 128)
            turned = jnp.transpose(key_grad[:, lanes]).astype(bf16)
            for k in range(4):
                to = pl.multiple_of(i * 64 + (k // 2) * 32, 32)
                out_ref[2 * late + k % 2, pl.ds(to, 32), :] = turned[k * 32 : (k + 1) * 32]
        return carry

    lax.fori_loop(0, 16, emit, 0)


def rows_call(order, pieces, queries):
    return pl.pallas_call(
        rows_kernel,
        out_shape=jax.ShapeDtypeStruct((HEADS, KEY_ROWS + GRAD_ROWS, DI), bf16),
        in_specs=[
            pl.BlockSpec(memory_space=pltpu.SMEM),
            *[pl.BlockSpec(memory_space=pl.ANY)] * (2 * PIECES),
            pl.BlockSpec(memory_space=pltpu.VMEM),
        ],
        out_specs=pl.BlockSpec(memory_space=pltpu.VMEM),
        scratch_shapes=[
            pltpu.VMEM((32, KW + DI, 128), bf16),
            pltpu.VMEM((832, LENGTH), bf16),
            pltpu.VMEM((2, 2, ROWS // 2, 640), bf16),
            pltpu.VMEM((2, IROWS, DI), bf16),
            pltpu.VMEM((ROWS, LENGTH), f32),
            pltpu.VMEM((ROWS, 128), f32),
            pltpu.VMEM((ROWS, 128), f32),
            pltpu.VMEM((2, IROWS, DI), f32),
            pltpu.VMEM((GROUP, LENGTH), f32),
            pltpu.VMEM((GROUP, LENGTH), f32),
            pltpu.VMEM((GROUP, LENGTH), f32),
            pltpu.VMEM((IROWS, DI), f32),
            pltpu.VMEM((DI, LENGTH), f32),
            pltpu.SemaphoreType.DMA((32,)),
        ],
        compiler_params=pltpu.CompilerParams(vmem_limit_bytes=58 * 1024 * 1024),
        name="rows_work",
    )(order, *pieces, queries)


def spread_kernel(order_ref, got_ref, out_ref, sums):
    first, _ = own_block(order_ref)
    total = got_ref[0, 0:KEY_ROWS].astype(f32)
    for src in range(1, HEADS):
        total = total + got_ref[src, 0:KEY_ROWS].astype(f32)
    sums[0:KEY_ROWS] = total.astype(bf16)
    sums[KEY_ROWS:] = jnp.zeros((32, DI), bf16)

    def put(d, carry):
        slot = order_ref[2 * d] - first
        slot = jnp.where((slot >= 0) & (slot < 64), slot, 32)
        out_ref[d] = sums[pl.ds(pl.multiple_of(slot * 32, 32), 32)]
        return carry

    lax.fori_loop(0, 64, put, 0, unroll=8)


def spread_call(order, got):
    return pl.pallas_call(
        spread_kernel,
        out_shape=jax.ShapeDtypeStruct((64, 32, DI), bf16),
        in_specs=[
            pl.BlockSpec(memory_space=pltpu.SMEM),
            pl.BlockSpec(memory_space=pltpu.VMEM),
        ],
        out_specs=pl.BlockSpec(memory_space=pltpu.VMEM),
        scratch_shapes=[pltpu.VMEM((KEY_ROWS + 32, DI), bf16)],
        name="spread_keys",
    )(order, got)


def work(block_order, main_query, latent_key, index_query, index_weight, index_key):
    shard = jnp.concatenate([latent_key, index_key], axis=0)
    pieces = gather_keys(shard)

    weights = jnp.pad(index_weight, ((0, 0), (0, 128 - index_weight.shape[1])))
    rows = jnp.concatenate([main_query, index_query.reshape(128, INDEX_LANES), weights], axis=1)
    rows = rows.reshape(2, HEADS, GROUP, ALL_LANES).swapaxes(0, 1)
    queries = lax.all_to_all(rows, "head", split_axis=0, concat_axis=0, tiled=True)

    sent = rows_call(block_order, pieces, queries)
    got = lax.all_to_all(sent, "head", split_axis=0, concat_axis=0, tiled=True)
    parts = lax.all_to_all(spread_call(block_order, got), CTX, split_axis=0, concat_axis=0, tiled=True)
    grad_key = jnp.sum(parts.astype(f32), axis=0)

    grads = got[:, KEY_ROWS:].reshape(HEADS, 2, 9, GROUP, DI).transpose(1, 0, 3, 2, 4)
    grads = grads.reshape(128, 9, DI)
    small = grads[:, 8]
    row_loss = jnp.sum(small[:, 8:11].astype(f32), axis=1)
    return (row_loss, grads[:, 0:8], small[:, 0:8], grad_key)


def onward(piece, axis):
    n = lax.axis_size(axis)
    return lax.ppermute(piece, axis, [(i, (i + 1) % n) for i in range(n)])


def backward(piece, axis):
    n = lax.axis_size(axis)
    return lax.ppermute(piece, axis, [(i, (i - 1) % n) for i in range(n)])


def swapped(piece):
    return lax.ppermute(piece, "ctx_2", [(0, 1), (1, 0)])


def sent_to_all(piece, axis):
    copies = jnp.broadcast_to(piece, (lax.axis_size(axis), *piece.shape))
    return lax.all_to_all(copies, axis, split_axis=0, concat_axis=0, tiled=True)


def gather_keys(shard):
    core = lax.axis_index("ctx_2")
    top, bottom = shard[:HALF_ROWS], shard[HALF_ROWS:]
    mine = jnp.where(core == 0, top, bottom)
    given = jnp.where(core == 0, bottom, top)
    block = jnp.stack([mine, swapped(given)])
    first, second = block[:, :STRIP], block[:, STRIP:]

    z, y = "ctx_1", "ctx_0"
    planes = sent_to_all(first, z)
    h1, g1 = backward(second, y), onward(second, y)
    g2 = lax.ppermute(second, y, [(i, (i + 2) % 4) for i in range(4)])
    rows = jnp.stack([second, h1, g2, g1])
    b1, f1 = backward(rows, z), onward(rows, z)
    down1, up1 = backward(planes, y), onward(planes, y)
    b2, f2 = backward(b1, z), onward(f1, z)
    up2, down2 = onward(up1[:, :, :STRIP_CUT], y), backward(down1[:, :, STRIP_CUT:], y)
    b3, f3 = backward(b2, z), onward(f2, z)
    f4, b4 = onward(f3[:, :, :REST_CUT], z), backward(b3[:, :, REST_CUT:], z)
    own = [planes, down1, up1, up2, down2, rows, b1, b2, b3, f3, f2, f1, f4, b4]
    return own + [swapped(piece) for piece in own]


def solution(mesh):
    split = Mesh(
        mesh.devices.reshape(4, 8, 2, mesh.shape["head"]), ("ctx_0", "ctx_1", "ctx_2", "head")
    )
    in_specs = (
        P(),
        P(CTX, "head"),
        P(None, CTX),
        P(CTX, "head", None),
        P(CTX, "head"),
        P(None, CTX),
    )
    out_specs = (P(CTX), P(CTX, "head", None), P(CTX, "head"), P(CTX_HEAD, None))
    return jax.shard_map(work, mesh=split, in_specs=in_specs, out_specs=out_specs, check_vma=False)
```

```python
import math

import jax
import jax.numpy as jnp
from jax import lax
from jax.experimental import pallas as pl
from jax.experimental.pallas import tpu as pltpu
from jax.sharding import Mesh
from jax.sharding import PartitionSpec as P


HM = 64
HI = 32
DI = 128
KW = 576
HEAD_QK = 192
BLOCK = 64
LENGTH = 4096
HALF = LENGTH // 2
CTX = ("ctx_0", "ctx_1", "ctx_2")
CTX_HEAD = ("ctx_0", "ctx_1", "ctx_2", "head")
HEADS = 4
GROUP = 16
MAIN_LANES = HM // HEADS * KW
INDEX_LANES = HI // HEADS * DI
ALL_LANES = MAIN_LANES + INDEX_LANES + 128
TILE = 256
TILES = LENGTH // TILE
WIDE = 512
ROWS = HM * GROUP
IROWS = HI * GROUP
KEY_ROWS = 1024
GRAD_ROWS = 9 * 2 * GROUP
HALF_ROWS = (KW + DI) // 2
STRIP = 176
STRIP_CUT = 96
REST = HALF_ROWS - STRIP
REST_CUT = 96
PIECES = 14
masked_value = -1e30
SCORE_EXP2 = math.log2(math.e) / math.sqrt(HEAD_QK)
f32 = jnp.float32
bf16 = jnp.bfloat16


def sources(y, z):
    if y == 2:
        first = [(3, 0, STRIP_CUT), (4, STRIP_CUT, STRIP - STRIP_CUT)]
    else:
        first = [({0: 0, 1: 1, 3: 2}[y], 0, STRIP)]
    if z == 4:
        rest = [(12, STRIP, REST_CUT), (13, STRIP + REST_CUT, REST - REST_CUT)]
    else:
        rest = [({0: 5, 1: 6, 2: 7, 3: 8, 5: 9, 6: 10, 7: 11}[z], STRIP, REST)]
    return first, rest


def nt_dot(a, b):
    return lax.dot_general(a, b, (((1,), (1,)), ((), ())), preferred_element_type=f32)


def own_block(order_ref):
    y, z, core = (lax.axis_index(axis) for axis in CTX)
    own = order_ref[((y * 8 + z) * 2 + core) * 2]
    first = jnp.where(own >= 64, 64, 0)
    return first, own - first


def rows_kernel(order_ref, *refs):
    pieces = refs[: 2 * PIECES]
    q_ref, out_ref = refs[2 * PIECES : 2 * PIECES + 2]
    (
        raw, keys, q_all, qi_all, scores, best, total, w_all, target, logits, slope, gsum,
        key_grad, sems,
    ) = refs[2 * PIECES + 2 :]
    y_own, z_own, core_own = (lax.axis_index(axis) for axis in CTX)
    h_own = lax.axis_index("head")
    first, c_own = own_block(order_ref)
    own_half = pl.multiple_of(core_own * HALF_ROWS, 16)
    other_half = pl.multiple_of((1 - core_own) * HALF_ROWS, 16)

    for y in range(4):
        for z in range(8):
            for core in range(2):
                y_from, z_from = (y_own + y) % 4, (z_own + z) % 8
                place = (y_from * 8 + z_from) * 2 + (core_own + core) % 2
                slot = order_ref[2 * place] - first

                @pl.when((slot >= 0) & (slot < 64))
                def _():
                    for parts, block in zip(sources(y, z), (z_from, y)):
                        for piece, at, size in parts:
                            for kind, half in ((0, own_half), (1, other_half)):
                                pltpu.make_async_copy(
                                    pieces[kind * PIECES + piece].at[block, core ^ kind],
                                    raw.at[slot, pl.ds(half + at, size), :],
                                    sems.at[slot],
                                ).start()

    def arrived(n):
        pltpu.make_async_copy(raw.at[n], raw.at[n], sems.at[n]).wait()

    keys[:, 0:64, :] = jnp.zeros((LENGTH // WIDE, 64, WIDE), bf16)
    keys[:, 640:704, :] = jnp.zeros((LENGTH // WIDE, 64, WIDE), bf16)

    for e in range(2):
        for src in range(HEADS):
            for i in range(8):
                at = (src * 8 + i) * GROUP
                for parity in range(2):
                    lane = i * 2 * KW + parity * (KW - 64)
                    q_all[e, parity, at : at + GROUP, :] = q_ref[src, e, :, lane : lane + 640]
                lane = MAIN_LANES + i * DI
                qi_all[e, at : at + GROUP, :] = q_ref[src, e, :, lane : lane + DI]
                lane = MAIN_LANES + INDEX_LANES
                column = q_ref[src, e, :, lane : lane + 128].astype(f32)[:, i : i + 1]
                w_all[e, at : at + GROUP, :] = jnp.broadcast_to(column, (GROUP, DI))

    take = lax.broadcasted_iota(jnp.int32, (256, 256), 0)
    give = lax.broadcasted_iota(jnp.int32, (256, 256), 1)
    source = jnp.where(give // 64 == 1, give + 64, jnp.where(give // 64 == 2, give - 64, give))
    shuffle = jnp.where(take == source, 1.0, 0.0).astype(bf16)

    def sort_pair(i, carry):
        arrived(2 * i)
        arrived(2 * i + 1)
        both = jnp.concatenate([raw[2 * i], raw[2 * i + 1]], axis=1)
        mixed = jnp.dot(both, shuffle, preferred_element_type=f32).astype(bf16)
        for late in range(2):
            n = late * (HALF // WIDE) + i // 4
            lanes = pl.ds(pl.multiple_of(i % 4 * 128, 128), 128)
            keys[n, 64:640, lanes] = mixed[0:KW, late * 128 : late * 128 + 128]
            keys[n, 704:832, lanes] = mixed[KW:, late * 128 : late * 128 + 128]
        return carry

    lax.fori_loop(0, 16, sort_pair, 0)

    key_grad[...] = jnp.zeros((DI, LENGTH), f32)

    for e in range(2):
        row_pos = lax.broadcasted_iota(jnp.int32, (GROUP, 1), 0) + h_own * GROUP
        row_pos = row_pos + (c_own if e == 0 else 63 - c_own) * BLOCK

        def key_pos(at, width):
            lane = lax.broadcasted_iota(jnp.int32, (1, width), 1) + at
            late_lane = lane - HALF
            late_pos = (63 - late_lane // BLOCK) * BLOCK + late_lane % BLOCK
            return jnp.where(lane < HALF, lane, late_pos)

        early_tiles = c_own // 4 + 1 if e == 0 else TILES // 2
        late_tiles = 0 if e == 0 else TILES // 2 - c_own // 4

        def tile_at(j):
            if e == 0:
                return pl.multiple_of(j * TILE, TILE)
            return pl.multiple_of(jnp.where(j < TILES // 2, j, j + c_own // 4) * TILE, TILE)

        steps = early_tiles + late_tiles

        best[...] = jnp.full((ROWS, 128), masked_value, f32)
        total[...] = jnp.zeros((ROWS, 128), f32)
        target[...] = jnp.zeros((GROUP, LENGTH), f32)
        logits[...] = jnp.full((GROUP, LENGTH), masked_value, f32)

        wide_steps = c_own // 8 + 1 if e == 0 else LENGTH // WIDE - c_own // 8

        def score_step(j, carry):
            at = j if e == 0 else jnp.where(j < HALF // WIDE, j, j + c_own // 8)
            at = pl.multiple_of(at * WIDE, WIDE)
            visible = key_pos(at, WIDE) <= row_pos
            for parity in range(2):
                k = keys[at // WIDE, 64 * (1 - parity) : 64 * (1 - parity) + 640, :]
                s = jnp.dot(q_all[e, parity], k, preferred_element_type=f32)
                s = jnp.where(visible[None], s.reshape(HM // 2, GROUP, WIDE), masked_value)
                s = s.reshape(ROWS // 2, WIDE)
                r = slice(parity * (ROWS // 2), (parity + 1) * (ROWS // 2))
                for i in range(WIDE // 128):
                    scores[at // 128 + i, r] = s[:, i * 128 : (i + 1) * 128]
                top = jnp.maximum(s[:, 0:128], s[:, 128:256])
                best[r] = jnp.maximum(best[r], jnp.maximum(top, jnp.maximum(s[:, 256:384], s[:, 384:512])))
            return carry

        lax.fori_loop(0, wide_steps, score_step, 0)

        def top_step(g, carry):
            r = pl.ds(pl.multiple_of(g * 128, 128), 128)
            best[r] = jnp.broadcast_to(jnp.max(best[r], axis=1, keepdims=True), (128, 128))
            return carry

        lax.fori_loop(0, ROWS // 128, top_step, 0)

        def exp_step(j, carry):
            at = tile_at(j)
            for g in range(ROWS // 128):
                r = slice(g * 128, (g + 1) * 128)
                top = best[r]
                part = total[r]
                for half in range(TILE // 128):
                    n = at // 128 + half
                    raised = jnp.exp2((scores[n, r] - top) * SCORE_EXP2)
                    scores[n, r] = raised
                    part = part + raised
                total[r] = part
            return carry

        lax.fori_loop(0, steps, exp_step, 0)

        def total_step(g, carry):
            r = pl.ds(pl.multiple_of(g * 128, 128), 128)
            whole = jnp.sum(total[r], axis=1, keepdims=True)
            total[r] = jnp.broadcast_to((1.0 / HM) / whole, (128, 128))
            return carry

        lax.fori_loop(0, ROWS // 128, total_step, 0)

        def index_logits(at):
            act = jnp.dot(
                qi_all[e], keys[at // WIDE, 704:832, pl.ds(pl.multiple_of(at % WIDE, TILE), TILE)], preferred_element_type=f32
            )
            out = jnp.zeros((GROUP, TILE), f32)
            for h in range(HI):
                r = slice(h * GROUP, (h + 1) * GROUP)
                w = w_all[e, r]
                out = out + jnp.maximum(act[r], 0.0) * jnp.concatenate([w, w], axis=1)
            return out

        def target_step(j, carry):
            at = tile_at(j)
            lanes = pl.ds(at, TILE)
            acc = [jnp.zeros((GROUP, 128), f32) for _ in range(TILE // 128)]
            for h in range(HM):
                r = slice(h * GROUP, (h + 1) * GROUP)
                share = total[r]
                for half in range(TILE // 128):
                    acc[half] = acc[half] + scores[at // 128 + half, r] * share
            target[:, lanes] = jnp.concatenate(acc, axis=1)
            visible = key_pos(at, TILE) <= row_pos
            logits[:, lanes] = jnp.where(visible, index_logits(at), masked_value)
            return carry

        lax.fori_loop(0, steps, target_step, 0)

        masked = logits[...]
        visible = masked > 0.5 * masked_value
        top_logit = jnp.max(masked, axis=1, keepdims=True)
        lse = top_logit + jnp.log(jnp.sum(jnp.exp(masked - top_logit), axis=1, keepdims=True))
        loss = jnp.sum(jnp.where(visible, target[...] * (lse - masked), 0.0), axis=1, keepdims=True)
        rounded = jnp.where(visible, jnp.exp(masked - lse) - target[...], 0.0).astype(bf16)
        slope[...] = rounded.astype(f32)

        gsum[...] = jnp.zeros((IROWS, DI), f32)
        q_float = qi_all[e].astype(f32)
        weighted = jnp.transpose(q_float * w_all[e]).astype(bf16)

        def back_step(j, carry):
            at = j if e == 0 else jnp.where(j < HALF // WIDE, j, j + c_own // 8)
            lanes = pl.ds(pl.multiple_of(at * WIDE, WIDE), WIDE)
            k = keys[at, 704:832, :]
            act = jnp.dot(qi_all[e], k, preferred_element_type=f32)
            through = jnp.where(
                act.reshape(HI, GROUP, WIDE) > 0.0, slope[:, lanes][None], 0.0
            ).reshape(IROWS, WIDE).astype(bf16)
            gsum[...] += nt_dot(through, k)
            key_grad[:, lanes] += jnp.dot(weighted, through, preferred_element_type=f32)
            return carry

        lax.fori_loop(0, wide_steps, back_step, 0)

        grads = (gsum[...] * w_all[e]).astype(bf16)
        column = jnp.sum(gsum[...] * q_float, axis=1, keepdims=True)
        lane = lax.broadcasted_iota(jnp.int32, (GROUP, 128), 1)
        high = loss.astype(bf16).astype(f32)
        middle = (loss - high).astype(bf16).astype(f32)
        low = loss - high - middle
        extra = jnp.where(lane == 8, high, jnp.where(lane == 9, middle, jnp.where(lane == 10, low, 0.0)))
        for dst in range(HEADS):
            small = extra
            for i in range(8):
                at = (dst * 8 + i) * GROUP
                to = KEY_ROWS + (e * 9 + i) * GROUP
                out_ref[dst, to : to + GROUP, :] = grads[at : at + GROUP]
                small = jnp.where(lane == i, column[at : at + GROUP], small)
            to = KEY_ROWS + (e * 9 + 8) * GROUP
            out_ref[dst, to : to + GROUP, :] = small.astype(bf16)

    def emit(i, carry):
        for late in range(2):
            lanes = pl.ds(pl.multiple_of(late * HALF + i * 128, 128), 128)
            turned = jnp.transpose(key_grad[:, lanes]).astype(bf16)
            for k in range(4):
                to = pl.multiple_of(i * 64 + (k // 2) * 32, 32)
                out_ref[2 * late + k % 2, pl.ds(to, 32), :] = turned[k * 32 : (k + 1) * 32]
        return carry

    lax.fori_loop(0, 16, emit, 0)


def rows_call(order, pieces, queries):
    return pl.pallas_call(
        rows_kernel,
        out_shape=jax.ShapeDtypeStruct((HEADS, KEY_ROWS + GRAD_ROWS, DI), bf16),
        in_specs=[
            pl.BlockSpec(memory_space=pltpu.SMEM),
            *[pl.BlockSpec(memory_space=pl.ANY)] * (2 * PIECES),
            pl.BlockSpec(memory_space=pltpu.VMEM),
        ],
        out_specs=pl.BlockSpec(memory_space=pltpu.VMEM),
        scratch_shapes=[
            pltpu.VMEM((32, KW + DI, 128), bf16),
            pltpu.VMEM((LENGTH // WIDE, 832, WIDE), bf16),
            pltpu.VMEM((2, 2, ROWS // 2, 640), bf16),
            pltpu.VMEM((2, IROWS, DI), bf16),
            pltpu.VMEM((LENGTH // 128, ROWS, 128), f32),
            pltpu.VMEM((ROWS, 128), f32),
            pltpu.VMEM((ROWS, 128), f32),
            pltpu.VMEM((2, IROWS, DI), f32),
            pltpu.VMEM((GROUP, LENGTH), f32),
            pltpu.VMEM((GROUP, LENGTH), f32),
            pltpu.VMEM((GROUP, LENGTH), f32),
            pltpu.VMEM((IROWS, DI), f32),
            pltpu.VMEM((DI, LENGTH), f32),
            pltpu.SemaphoreType.DMA((32,)),
        ],
        compiler_params=pltpu.CompilerParams(vmem_limit_bytes=58 * 1024 * 1024),
        name="rows_work",
    )(order, *pieces, queries)


def spread_kernel(order_ref, got_ref, out_ref, sums):
    first, _ = own_block(order_ref)
    total = got_ref[0, 0:KEY_ROWS].astype(f32)
    for src in range(1, HEADS):
        total = total + got_ref[src, 0:KEY_ROWS].astype(f32)
    sums[0:KEY_ROWS] = total.astype(bf16)
    sums[KEY_ROWS:] = jnp.zeros((32, DI), bf16)

    def put(d, carry):
        slot = order_ref[2 * d] - first
        slot = jnp.where((slot >= 0) & (slot < 64), slot, 32)
        out_ref[d] = sums[pl.ds(pl.multiple_of(slot * 32, 32), 32)]
        return carry

    lax.fori_loop(0, 64, put, 0, unroll=8)


def spread_call(order, got):
    return pl.pallas_call(
        spread_kernel,
        out_shape=jax.ShapeDtypeStruct((64, 32, DI), bf16),
        in_specs=[
            pl.BlockSpec(memory_space=pltpu.SMEM),
            pl.BlockSpec(memory_space=pltpu.VMEM),
        ],
        out_specs=pl.BlockSpec(memory_space=pltpu.VMEM),
        scratch_shapes=[pltpu.VMEM((KEY_ROWS + 32, DI), bf16)],
        name="spread_keys",
    )(order, got)


def work(block_order, main_query, latent_key, index_query, index_weight, index_key):
    shard = jnp.concatenate([latent_key, index_key], axis=0)
    pieces = gather_keys(shard)

    weights = jnp.pad(index_weight, ((0, 0), (0, 128 - index_weight.shape[1])))
    rows = jnp.concatenate([main_query, index_query.reshape(128, INDEX_LANES), weights], axis=1)
    rows = rows.reshape(2, HEADS, GROUP, ALL_LANES).swapaxes(0, 1)
    queries = lax.all_to_all(rows, "head", split_axis=0, concat_axis=0, tiled=True)

    sent = rows_call(block_order, pieces, queries)
    got = lax.all_to_all(sent, "head", split_axis=0, concat_axis=0, tiled=True)
    parts = lax.all_to_all(spread_call(block_order, got), CTX, split_axis=0, concat_axis=0, tiled=True)
    grad_key = jnp.sum(parts.astype(f32), axis=0)

    grads = got[:, KEY_ROWS:].reshape(HEADS, 2, 9, GROUP, DI).transpose(1, 0, 3, 2, 4)
    grads = grads.reshape(128, 9, DI)
    small = grads[:, 8]
    row_loss = jnp.sum(small[:, 8:11].astype(f32), axis=1)
    return (row_loss, grads[:, 0:8], small[:, 0:8], grad_key)


def onward(piece, axis):
    n = lax.axis_size(axis)
    return lax.ppermute(piece, axis, [(i, (i + 1) % n) for i in range(n)])


def backward(piece, axis):
    n = lax.axis_size(axis)
    return lax.ppermute(piece, axis, [(i, (i - 1) % n) for i in range(n)])


def swapped(piece):
    return lax.ppermute(piece, "ctx_2", [(0, 1), (1, 0)])


def sent_to_all(piece, axis):
    copies = jnp.broadcast_to(piece, (lax.axis_size(axis), *piece.shape))
    return lax.all_to_all(copies, axis, split_axis=0, concat_axis=0, tiled=True)


def gather_keys(shard):
    core = lax.axis_index("ctx_2")
    top, bottom = shard[:HALF_ROWS], shard[HALF_ROWS:]
    mine = jnp.where(core == 0, top, bottom)
    given = jnp.where(core == 0, bottom, top)
    block = jnp.stack([mine, swapped(given)])
    first, second = block[:, :STRIP], block[:, STRIP:]

    z, y = "ctx_1", "ctx_0"
    planes = sent_to_all(first, z)
    h1, g1 = backward(second, y), onward(second, y)
    g2 = lax.ppermute(second, y, [(i, (i + 2) % 4) for i in range(4)])
    rows = jnp.stack([second, h1, g2, g1])
    b1, f1 = backward(rows, z), onward(rows, z)
    down1, up1 = backward(planes, y), onward(planes, y)
    b2, f2 = backward(b1, z), onward(f1, z)
    b3, f3 = backward(b2, z), onward(f2, z)
    up2, down2 = onward(up1[:, :, :STRIP_CUT], y), backward(down1[:, :, STRIP_CUT:], y)
    f4, b4 = onward(f3[:, :, :REST_CUT], z), backward(b3[:, :, REST_CUT:], z)
    own = [planes, down1, up1, up2, down2, rows, b1, b2, b3, f3, f2, f1, f4, b4]
    return own + [swapped(piece) for piece in own]


def solution(mesh):
    split = Mesh(
        mesh.devices.reshape(4, 8, 2, mesh.shape["head"]), ("ctx_0", "ctx_1", "ctx_2", "head")
    )
    in_specs = (
        P(),
        P(CTX, "head"),
        P(None, CTX),
        P(CTX, "head", None),
        P(CTX, "head"),
        P(None, CTX),
    )
    out_specs = (P(CTX), P(CTX, "head", None), P(CTX, "head"), P(CTX_HEAD, None))
    return jax.shard_map(work, mesh=split, in_specs=in_specs, out_specs=out_specs, check_vma=False)
```
